256 devices in a mesh: ctx: 32 (over z_hi, y, core), tp: 8 (over z_lo, x).
Axes of the slice: x: 4, y: 4, z: 8 (z_hi: 4, z_lo: 2; z = z_hi * 2 + z_lo), core: 2. Of those that a mesh axis runs over, the one named last changes fastest.
Arguments:
- queries: bfloat16 [4096, 8192], P('ctx', 'tp'), may hold values from -256 to 256
- keys: bfloat16 [4096, 1024], P(('ctx', 'tp')), may hold values from -6.5 to 6.5
- values: bfloat16 [4096, 1024], P(('ctx', 'tp')), may hold values from -6 to 6
- output_gradient: bfloat16 [4096, 8192], P('ctx', 'tp'), may hold values from -6 to 6
- span_order: int32 [64], replicated, may hold values from 0 to 63, as said below
Outputs:
- query_grad: bfloat16 [4096, 8192], P('ctx', 'tp')
- key_gradient_rows: bfloat16 [4096, 1024], P(('ctx', 'tp'))
- value_gradient_rows: bfloat16 [4096, 1024], P(('ctx', 'tp'))
The draws below stay inside these ranges and needn't reach their ends.
Inputs may be any that keep to these rules, and one draw needn't show every extreme that they name: `span_order`: each value 0 to 63 appears once; entries 2d and 2d + 1 sum to 63.
All inputs are finite; a program needn't handle non-finite values.
Results may differ from the reference program's by a relative error of at most 0.0073.
Values may be sent and summed in bfloat16 or wider, within the bound.
A program may use at most 64 MiB of HBM per device.

```python
import jax
import jax.numpy as jnp
from jax import lax

HEAD_SIZE = 128
QUERY_HEADS = 64
KEY_VALUE_HEADS = 8
TOK_DEV = 128
SPAN = 64
SEQUENCE_TOKENS = 4096


def joint_sample(key):
    base = jax.random.fold_in(key, 7)
    first_half, second = jax.random.split(base, 2)
    key_value_pairs = jnp.clip(jax.random.normal(first_half, (SEQUENCE_TOKENS, KEY_VALUE_HEADS, HEAD_SIZE), jnp.float32), -6.0, 6.0)
    query_vals = jnp.clip(jax.random.normal(second, (SEQUENCE_TOKENS, QUERY_HEADS, HEAD_SIZE), jnp.float32), -6.0, 6.0)
    query_vals = jnp.clip(query_vals, -256.0, 256.0)
    return (query_vals, key_value_pairs)


def draw_queries(key, part):
    return joint_sample(key)[0].reshape(SEQUENCE_TOKENS, QUERY_HEADS * HEAD_SIZE).astype(jnp.bfloat16)


def draw_keys(key, part):
    return joint_sample(key)[1].reshape(SEQUENCE_TOKENS, KEY_VALUE_HEADS * HEAD_SIZE).astype(jnp.bfloat16)


def draw_span_order(key, part):
    pairs = SEQUENCE_TOKENS // TOK_DEV
    perm = jax.random.permutation(jax.random.fold_in(key, 11), pairs).astype(jnp.int32)
    flips = jax.random.randint(jax.random.fold_in(key, 13), (pairs,), 0, 2)
    leading = jnp.where(flips == 0, perm, 2 * pairs - 1 - perm)
    trailing = 2 * pairs - 1 - leading
    return jnp.stack([leading, trailing], axis=1).reshape(-1).astype(jnp.int32)


def block_levels(key, dims, pieces, least, top_value):
    loudness, own = 1.0, jax.random.fold_in(key, 6)
    for axis_at, parts in pieces:
        steps = jnp.exp(jax.random.uniform(jax.random.fold_in(own, axis_at), (parts,), jnp.float32, least / len(pieces), top_value / len(pieces)))
        loudness = loudness * jnp.repeat(steps, dims[axis_at] // parts).reshape([-1 if axis == axis_at else 1 for axis in range(len(dims))])
    return loudness


def gaussian(key, shape, deviation, bound, cuts=(), kind=jnp.bfloat16):
    gain = block_levels(key, shape, cuts, -0.22, 0.18) if cuts else 1.0
    values = jax.random.normal(key, shape, jnp.float32) * deviation * gain
    return jnp.minimum(jnp.maximum(values, -bound), bound).astype(kind)


def setup_inputs(seed: int = 0) -> dict:
    key_of = jax.random.split(jax.random.key(seed), 6)
    queries = draw_queries(jax.random.fold_in(key_of[5], 71), 0)
    keys = draw_keys(jax.random.fold_in(key_of[5], 71), 0)
    values = gaussian(key_of[2], (SEQUENCE_TOKENS, KEY_VALUE_HEADS * HEAD_SIZE), 1.0, 6.0, ((0, 256),))
    output_gradient = gaussian(key_of[3], (SEQUENCE_TOKENS, QUERY_HEADS * HEAD_SIZE), 1.0, 6.0, ((0, 32), (1, 8)))
    span_order = draw_span_order(jax.random.fold_in(key_of[5], 71), 0)
    return dict(queries=queries, keys=keys, values=values, output_gradient=output_gradient, span_order=span_order)


def reference(queries, keys, values, output_gradient, span_order):
    scale = HEAD_SIZE ** -0.5
    head_group = QUERY_HEADS // KEY_VALUE_HEADS
    rows = jnp.arange(SEQUENCE_TOKENS, dtype=jnp.int32)
    pos = span_order[rows // SPAN] * SPAN + rows % SPAN
    visible = pos[:, None] >= pos[None, :]
    query_head_rows = queries.reshape(SEQUENCE_TOKENS, KEY_VALUE_HEADS, head_group, HEAD_SIZE).transpose(1, 2, 0, 3)
    gradient_heads = output_gradient.reshape(SEQUENCE_TOKENS, KEY_VALUE_HEADS, head_group, HEAD_SIZE).transpose(1, 2, 0, 3)
    key_head_rows = keys.reshape(SEQUENCE_TOKENS, KEY_VALUE_HEADS, HEAD_SIZE).transpose(1, 0, 2)
    value_head_rows = values.reshape(SEQUENCE_TOKENS, KEY_VALUE_HEADS, HEAD_SIZE).transpose(1, 0, 2)

    def one_group(items):
        q_group, g_group, k_group, v_group = items

        def one_head(carry, pair):
            q_head, g_head = pair
            score = jnp.dot(q_head, k_group.T, preferred_element_type=jnp.float32) * scale
            score = jnp.where(visible, score, -jnp.inf)
            top = jnp.max(score, axis=1, keepdims=True)
            expo = jnp.exp(score - top)
            prob = expo / jnp.sum(expo, axis=1, keepdims=True)
            dprob = jnp.dot(g_head, v_group.T, preferred_element_type=jnp.float32)
            delta = jnp.sum(prob * dprob, axis=1, keepdims=True)
            dscore = (prob * (dprob - delta) * scale).astype(jnp.bfloat16)
            weights = prob.astype(jnp.bfloat16)
            dquery = jnp.dot(dscore, k_group, preferred_element_type=jnp.float32)
            key_gradient = carry[0] + jnp.dot(dscore.T, q_head, preferred_element_type=jnp.float32)
            value_gradient = carry[1] + jnp.dot(weights.T, g_head, preferred_element_type=jnp.float32)
            return (key_gradient, value_gradient), dquery

        zeros = jnp.zeros((SEQUENCE_TOKENS, HEAD_SIZE), jnp.float32)
        (key_gradient, value_gradient), dquery = lax.scan(one_head, (zeros, zeros), (q_group, g_group))
        return dquery, key_gradient, value_gradient

    dquery, key_gradient, value_gradient = lax.map(one_group, (query_head_rows, gradient_heads, key_head_rows, value_head_rows))
    query_grad = dquery.transpose(2, 0, 1, 3).reshape(SEQUENCE_TOKENS, QUERY_HEADS * HEAD_SIZE).astype(jnp.bfloat16)
    key_gradient_rows = key_gradient.transpose(1, 0, 2).reshape(SEQUENCE_TOKENS, KEY_VALUE_HEADS * HEAD_SIZE).astype(jnp.bfloat16)
    value_gradient_rows = value_gradient.transpose(1, 0, 2).reshape(SEQUENCE_TOKENS, KEY_VALUE_HEADS * HEAD_SIZE).astype(jnp.bfloat16)
    return query_grad, key_gradient_rows, value_gradient_rows
```

```python
import functools
import math

import jax
import jax.numpy as jnp
from jax import lax
from jax.experimental import pallas as pl
from jax.experimental.pallas import tpu as pltpu
from jax.sharding import PartitionSpec as P

HEAD = 128
SPAN = 64
KV_HEADS = 8
NY = 4
NZ = 4
SCALE = HEAD**-0.5
EXPO = SCALE * math.log2(math.e)
NEG = -1e30
MESH = pl.DeviceIdType.MESH
F32 = jnp.float32
BF16 = jnp.bfloat16


def dot(a, b):
    return jnp.dot(a, b, preferred_element_type=F32)


def kernel(
    tps,
    heads,
    span,
    q_hbm,
    k_hbm,
    v_hbm,
    g_hbm,
    dq_out,
    k_out,
    v_out,
    kvst,
    kv,
    qs,
    gs,
    qn,
    gn,
    qt,
    gt,
    klo_s,
    kc_s,
    klot_s,
    kct_s,
    vlo_s,
    vc_s,
    s_s,
    d_s,
    s3_s,
    d3_s,
    st,
    st_in,
    cs,
    dqt,
    dk3,
    dqsend,
    dqrecv,
    out,
    ro,
    ry,
    rzo,
    rz,
    zs,
    fin,
    kvo,
    loc,
    a2a,
    zsem_s,
    zsem_r,
    ysem_s,
    ysem_r,
    pair_s,
    pair_r,
    yo_s,
    yo_r,
    yf_s,
    yf_r,
    zr_s,
    zr_r,
):
    rows = heads * SPAN
    toks = 2 * SPAN
    tt = toks // tps
    c = lax.axis_index("ctx")
    t = lax.axis_index("tp")
    core = lax.rem(c, 2)
    y = lax.rem(c // 2, NY)
    z = c // (2 * NY)

    def ctx_of(zz, yy, cc):
        return (zz * NY + yy) * 2 + cc

    y_up, y_dn, y_op = lax.rem(y + 1, NY), lax.rem(y + 3, NY), lax.rem(y + 2, NY)
    z_up, z_dn, z_op = lax.rem(z + 1, NZ), lax.rem(z + 3, NZ), lax.rem(z + 2, NZ)
    dev_yu, dev_yd = (ctx_of(z, y_up, core), t), (ctx_of(z, y_dn, core), t)
    dev_zu, dev_zd = (ctx_of(z_up, y, core), t), (ctx_of(z_dn, y, core), t)
    dev_pair = (ctx_of(z, y, 1 - core), t)

    def remote(src, dst, send, recv, device):
        return pltpu.make_async_remote_copy(
            src_ref=src,
            dst_ref=dst,
            send_sem=send,
            recv_sem=recv,
            device_id=device,
            device_id_type=MESH,
        )

    def landed(ref, sem):
        pltpu.make_async_copy(ref, ref, sem).wait()

    own_rows = pl.ds(pl.multiple_of(t * tt, tt), tt)
    for g in range(tps):
        cols = pl.ds(g * HEAD, HEAD)
        pltpu.make_async_copy(k_hbm.at[:, cols], kvst.at[g, 0], loc.at[0]).start()
        pltpu.make_async_copy(v_hbm.at[:, cols], kvst.at[g, 1], loc.at[0]).start()
    own_cols = pl.ds(pl.multiple_of(t * HEAD, HEAD), HEAD)
    pltpu.make_async_copy(k_hbm.at[:, own_cols], kv.at[z, y, 0, own_rows], a2a.at[1]).start()
    pltpu.make_async_copy(v_hbm.at[:, own_cols], kv.at[z, y, 1, own_rows], a2a.at[1]).start()
    for h in range(heads):
        cols = pl.ds(h * HEAD, HEAD)
        pltpu.make_async_copy(q_hbm.at[:, cols], qs.at[0, h], loc.at[1]).start()
        pltpu.make_async_copy(g_hbm.at[:, cols], gs.at[0, h], loc.at[2]).start()

    barrier = pltpu.get_barrier_semaphore()
    for o in range(1, tps):
        pl.semaphore_signal(
            barrier, inc=1, device_id=(c, lax.rem(t + o, tps)), device_id_type=MESH
        )
    for device in (dev_yu, dev_yd, dev_zu, dev_zd, dev_pair):
        pl.semaphore_signal(barrier, inc=1, device_id=device, device_id_type=MESH)
    landed(kvst, loc.at[0])
    pl.semaphore_wait(barrier, tps - 1 + 5)

    for o in range(1, tps):
        to = lax.rem(t + o, tps)
        remote(kvst.at[to], kv.at[z, y, :, own_rows], a2a.at[0], a2a.at[1], (c, to)).start()
    landed(qs.at[0], loc.at[1])
    q_copy = remote(qs.at[0], qs.at[1], pair_s.at[0], pair_r.at[0], dev_pair)
    q_copy.start()
    landed(gs.at[0], loc.at[2])
    g_copy = remote(gs.at[0], gs.at[1], pair_s.at[1], pair_r.at[1], dev_pair)
    g_copy.start()

    def spans(cc):
        s0, s1 = span[2 * cc], span[2 * cc + 1]
        return s0 > s1, jnp.minimum(s0, s1)

    devs = (c, ctx_of(z, y, 1 - core))
    flips, lows = zip(*[spans(d) for d in devs])

    def prepare(a):
        for src, normal, turned in ((qs, qn, qt), (gs, gn, gt)):
            first = src[a, :, 0:SPAN, :].reshape(rows, HEAD)
            second = src[a, :, SPAN : 2 * SPAN, :].reshape(rows, HEAD)
            lo = jnp.where(flips[a], second, first)
            hi = jnp.where(flips[a], first, second)
            normal[a, :, 0:HEAD] = lo
            normal[a, :, HEAD : 2 * HEAD] = hi
            turned[a, 0:HEAD, :] = lo.T
            turned[a, HEAD : 2 * HEAD, :] = hi.T

    def z_of(gi):
        return lax.rem(z + gi + (gi // 2) * (1 - 2 * (gi % 2)), NZ)

    def y_start(gi):
        b = kv.at[z_of(gi), y]
        remote(b, b, ysem_s.at[gi, 0], ysem_r.at[gi, 0], dev_yu).start()
        remote(b, b, ysem_s.at[gi, 1], ysem_r.at[gi, 1], dev_yd).start()

    def y_relay(gi):
        zg = z_of(gi)
        landed(kv.at[zg, y_dn], ysem_r.at[gi, 0])
        b = kv.at[zg, y_dn, 0]
        remote(b, b, ysem_s.at[gi, 2], ysem_r.at[gi, 2], dev_yu).start()
        landed(kv.at[zg, y_up], ysem_r.at[gi, 1])
        b = kv.at[zg, y_up, 1]
        remote(b, b, ysem_s.at[gi, 3], ysem_r.at[gi, 3], dev_yd).start()

    def y_finish(gi):
        zg = z_of(gi)
        landed(kv.at[zg, y_op, 0], ysem_r.at[gi, 2])
        landed(kv.at[zg, y_op, 1], ysem_r.at[gi, 3])

    own = kv.at[z, y]
    landed(own, a2a.at[1])
    remote(own, own, zsem_s.at[0], zsem_r.at[0], dev_zu).start()
    remote(own, own, zsem_s.at[1], zsem_r.at[1], dev_zd).start()
    y_start(0)

    prepare(0)

    def lohi(zg, yy, w):
        first, second = kv[zg, yy, w, 0:SPAN, :], kv[zg, yy, w, SPAN : 2 * SPAN, :]
        flip, _ = spans(ctx_of(zg, yy, core))
        return jnp.where(flip, second, first), jnp.where(flip, first, second)

    key_i = lax.broadcasted_iota(jnp.int32, (SPAN, rows), 0)
    tok_i = lax.rem(lax.broadcasted_iota(jnp.int32, (SPAN, rows), 1), SPAN)
    hidden = key_i > tok_i

    kself, vself = lohi(z, y, 0)[0], lohi(z, y, 1)[0]
    s3 = jnp.where(hidden, NEG, dot(kself, qt[0, 0:HEAD, :]))
    d3 = dot(vself, gt[0, 0:HEAD, :])
    s3_s[...] = s3
    d3_s[...] = d3
    m3 = jnp.max(s3, axis=0, keepdims=True)
    e3 = jnp.exp2((s3 - m3) * EXPO)
    none = jnp.full((1, rows), NEG, F32)
    zero = jnp.zeros((1, rows), F32)
    st[0, 0:1, :] = m3
    st[0, 1:2, :] = jnp.sum(e3, axis=0, keepdims=True)
    st[0, 2:3, :] = jnp.sum(e3 * d3, axis=0, keepdims=True)
    st[0, 3:4, :] = none
    st[0, 4:8, :] = jnp.zeros((4, rows), F32)
    st[1, 0:1, :] = none
    st[1, 1:3, :] = jnp.zeros((2, rows), F32)
    st[1, 3:4, :] = none
    st[1, 4:8, :] = jnp.zeros((4, rows), F32)

    q_copy.wait_recv()
    g_copy.wait_recv()
    prepare(1)

    landed(kv.at[z_dn, y], zsem_r.at[0])
    b = kv.at[z_dn, y, 0]
    remote(b, b, zsem_s.at[2], zsem_r.at[2], dev_zu).start()
    landed(kv.at[z_up, y], zsem_r.at[1])
    b = kv.at[z_up, y, 1]
    remote(b, b, zsem_s.at[3], zsem_r.at[3], dev_zd).start()
    y_start(1)
    y_start(2)
    y_relay(0)
    landed(kv.at[z_op, y, 0], zsem_r.at[2])
    landed(kv.at[z_op, y, 1], zsem_r.at[3])
    y_start(3)

    def picks(zg, a):
        return [spans(ctx_of(zg, yy, core))[1] < lows[a] for yy in range(NY)]

    def block(yy):
        return slice(yy * SPAN, (yy + 1) * SPAN)

    def scores(gi):
        zg = z_of(gi)
        k = [lohi(zg, yy, 0) for yy in range(NY)]
        v = [lohi(zg, yy, 1) for yy in range(NY)]
        for yy in range(NY):
            klo_s[gi, block(yy), :] = k[yy][0]
            vlo_s[gi, block(yy), :] = v[yy][0]
        klo, vlo = klo_s[gi], vlo_s[gi]
        klot_s[gi] = klo.T
        for a in range(2):
            pick = picks(zg, a)
            for yy in range(NY):
                for half, (src, dst) in ((0, (k, kc_s)), (1, (v, vc_s))):
                    lo, hi = src[yy]
                    none_ = jnp.zeros_like(lo)
                    dst[gi, a, block(yy), 0:HEAD] = jnp.where(pick[yy], lo, none_)
                    dst[gi, a, block(yy), HEAD : 2 * HEAD] = jnp.where(pick[yy], none_, hi)
            kc, vc = kc_s[gi, a], vc_s[gi, a]
            kct_s[gi, a] = kc.T
            s1 = dot(klo, qt[a, HEAD : 2 * HEAD, :])
            d1 = dot(vlo, gt[a, HEAD : 2 * HEAD, :])
            s2 = dot(kc, qt[a])
            d2 = dot(vc, gt[a])
            s_s[gi, a, 0] = s1
            d_s[gi, a, 0] = d1
            d_s[gi, a, 1] = d2
            parts = []
            for yy in range(NY):
                part = s2[block(yy), :]
                if a == 0:
                    here = jnp.logical_and(zg == z, yy == y)
                    part = jnp.where(jnp.logical_and(hidden, here), NEG, part)
                s_s[gi, a, 1, block(yy), :] = part
                parts.append(part)
            m_lo, l_lo, e_lo = st[a, 0:1, :], st[a, 1:2, :], st[a, 2:3, :]
            m_hi, l_hi, e_hi = st[a, 3:4, :], st[a, 4:5, :], st[a, 5:6, :]
            n_lo, n_hi = m_lo, jnp.maximum(m_hi, jnp.max(s1, axis=0, keepdims=True))
            for yy in range(NY):
                top = jnp.max(parts[yy], axis=0, keepdims=True)
                n_lo = jnp.maximum(n_lo, jnp.where(pick[yy], top, none))
                n_hi = jnp.maximum(n_hi, jnp.where(pick[yy], none, top))
            f_lo, f_hi = jnp.exp2((m_lo - n_lo) * EXPO), jnp.exp2((m_hi - n_hi) * EXPO)
            l_lo, e_lo, l_hi, e_hi = l_lo * f_lo, e_lo * f_lo, l_hi * f_hi, e_hi * f_hi
            e1 = jnp.exp2((s1 - n_hi) * EXPO)
            l_hi = l_hi + jnp.sum(e1, axis=0, keepdims=True)
            e_hi = e_hi + jnp.sum(e1 * d1, axis=0, keepdims=True)
            for yy in range(NY):
                e2 = jnp.exp2((parts[yy] - jnp.where(pick[yy], n_lo, n_hi)) * EXPO)
                total = jnp.sum(e2, axis=0, keepdims=True)
                inner = jnp.sum(e2 * d2[block(yy), :], axis=0, keepdims=True)
                l_lo = l_lo + jnp.where(pick[yy], total, zero)
                l_hi = l_hi + jnp.where(pick[yy], zero, total)
                e_lo = e_lo + jnp.where(pick[yy], inner, zero)
                e_hi = e_hi + jnp.where(pick[yy], zero, inner)
            st[a, 0:1, :] = n_lo
            st[a, 1:2, :] = l_lo
            st[a, 2:3, :] = e_lo
            st[a, 3:4, :] = n_hi
            st[a, 4:5, :] = l_hi
            st[a, 5:6, :] = e_hi

    def score_step(gi, carry):
        @pl.when(gi < NZ - 1)
        def _():
            y_relay(gi + 1)

        y_finish(gi)
        scores(gi)
        return carry

    lax.fori_loop(0, NZ, score_step, 0)

    st_copy = remote(st, st_in, pair_s.at[2], pair_r.at[2], dev_pair)
    st_copy.start()
    dqt[...] = jnp.zeros_like(dqt)
    st_copy.wait_recv()
    for a in range(2):
        for at in (0, 3):
            m0, l0, e0 = (st[a, at + i : at + i + 1, :] for i in range(3))
            m1, l1, e1 = (st_in[1 - a, at + i : at + i + 1, :] for i in range(3))
            m = jnp.maximum(m0, m1)
            f0, f1 = jnp.exp2((m0 - m) * EXPO), jnp.exp2((m1 - m) * EXPO)
            inv = 1.0 / (l0 * f0 + l1 * f1)
            cs[a, at : at + 1, :] = m
            cs[a, at + 1 : at + 2, :] = inv
            cs[a, at + 2 : at + 3, :] = (e0 * f0 + e1 * f1) * inv

    def weights(s, d, m, inv, delta):
        prob = jnp.exp2((s - m) * EXPO) * inv
        return prob.astype(BF16), (prob * (d - delta) * SCALE).astype(BF16)

    lo_stats = [[cs[a, i : i + 1, :] for i in range(3)] for a in range(2)]
    w3, ds3 = weights(s3_s[...], d3_s[...], *lo_stats[0])
    dk3[0] = dot(ds3, qn[0, :, 0:HEAD])
    dk3[1] = dot(w3, gn[0, :, 0:HEAD])
    dqt[0, 0:HEAD, :] = dot(lohi(z, y, 0)[0].T, ds3)

    def grads(gi):
        zg = z_of(gi)
        dlo, dhi = [[None] * NY, [None] * NY], [[None] * NY, [None] * NY]
        for a in range(2):
            pick = picks(zg, a)
            lo = [cs[a, i : i + 1, :] for i in range(3)]
            hi = [cs[a, 3 + i : 4 + i, :] for i in range(3)]
            w1, ds1 = weights(s_s[gi, a, 0], d_s[gi, a, 0], *hi)
            pairs = [
                weights(
                    s_s[gi, a, 1, block(yy), :],
                    d_s[gi, a, 1, block(yy), :],
                    *[jnp.where(pick[yy], l, h) for l, h in zip(lo, hi)],
                )
                for yy in range(NY)
            ]
            w2 = jnp.concatenate([p[0] for p in pairs], axis=0)
            ds2 = jnp.concatenate([p[1] for p in pairs], axis=0)
            for i, (x1, x2, wide) in enumerate(((ds1, ds2, qn), (w1, w2, gn))):
                one = dot(x1, wide[a, :, HEAD : 2 * HEAD])
                two = dot(x2, wide[a])
                for yy in range(NY):
                    left, right = two[block(yy), 0:HEAD], two[block(yy), HEAD : 2 * HEAD]
                    none_ = jnp.zeros_like(left)
                    new_lo = one[block(yy), :] + jnp.where(pick[yy], left, none_)
                    new_hi = jnp.where(pick[yy], none_, right)
                    if a == 0:
                        here = jnp.logical_and(zg == z, yy == y)
                        new_lo = new_lo + jnp.where(here, dk3[i], none_)
                        dlo[i][yy], dhi[i][yy] = new_lo, new_hi
                    else:
                        dlo[i][yy] = dlo[i][yy] + new_lo
                        dhi[i][yy] = dhi[i][yy] + new_hi
            dqt[a] += dot(kct_s[gi, a], ds2)
            dqt[a, HEAD : 2 * HEAD, :] += dot(klot_s[gi], ds1)
        for yy in range(NY):
            flip, _ = spans(ctx_of(zg, yy, core))
            for i in range(2):
                out[zg, yy, i, 0:SPAN, :] = jnp.where(flip, dhi[i][yy], dlo[i][yy]).astype(BF16)
                out[zg, yy, i, SPAN : 2 * SPAN, :] = jnp.where(
                    flip, dlo[i][yy], dhi[i][yy]
                ).astype(BF16)

    def plus(a, b):
        return (a.astype(F32) + b.astype(F32)).astype(BF16)

    def ry_opposite(gi):
        zg = z_of(gi)
        remote(out.at[zg, y_op, 0], ro.at[gi, 0], yo_s.at[gi, 0], yo_r.at[gi, 0], dev_yu).start()
        remote(out.at[zg, y_op, 1], ro.at[gi, 1], yo_s.at[gi, 1], yo_r.at[gi, 1], dev_yd).start()

    def ry_forward(gi):
        zg = z_of(gi)
        landed(ro.at[gi, 0], yo_r.at[gi, 0])
        out[zg, y_up, 0] = plus(out[zg, y_up, 0], ro[gi, 0])
        remote(out.at[zg, y_up], ry.at[gi, 0], yf_s.at[gi, 0], yf_r.at[gi, 0], dev_yu).start()
        landed(ro.at[gi, 1], yo_r.at[gi, 1])
        out[zg, y_dn, 1] = plus(out[zg, y_dn, 1], ro[gi, 1])
        remote(out.at[zg, y_dn], ry.at[gi, 1], yf_s.at[gi, 1], yf_r.at[gi, 1], dev_yd).start()

    def ry_total(gi):
        zg = z_of(gi)
        landed(ry.at[gi, 0], yf_r.at[gi, 0])
        landed(ry.at[gi, 1], yf_r.at[gi, 1])
        return out[zg, y].astype(F32) + ry[gi, 0].astype(F32) + ry[gi, 1].astype(F32)

    def z_opposite():
        zs[2] = ry_total(3).astype(BF16)
        remote(zs.at[2, 0], rzo.at[0], zr_s.at[0], zr_r.at[0], dev_zu).start()
        remote(zs.at[2, 1], rzo.at[1], zr_s.at[1], zr_r.at[1], dev_zd).start()

    def z_down():
        total = ry_total(2)
        landed(rzo.at[1], zr_r.at[1])
        zs[1, 0] = total[0].astype(BF16)
        zs[1, 1] = (total[1] + rzo[1].astype(F32)).astype(BF16)
        remote(zs.at[1], rz.at[1], zr_s.at[3], zr_r.at[3], dev_zd).start()

    def z_up_():
        total = ry_total(1)
        landed(rzo.at[0], zr_r.at[0])
        zs[0, 0] = (total[0] + rzo[0].astype(F32)).astype(BF16)
        zs[0, 1] = total[1].astype(BF16)
        remote(zs.at[0], rz.at[0], zr_s.at[2], zr_r.at[2], dev_zu).start()

    def grad_step(i, carry):
        gi = NZ - 1 - i
        grads(gi)
        ry_opposite(gi)

        @pl.when(i >= 1)
        def _():
            ry_forward(gi + 1)

        @pl.when(i == 2)
        def _():
            z_opposite()

        @pl.when(i == 3)
        def _():
            z_down()

        return carry

    lax.fori_loop(0, NZ, grad_step, 0)

    dqsend[...] = dqt[1].astype(BF16)
    ry_forward(0)
    dq_copy = remote(dqsend, dqrecv, pair_s.at[3], pair_r.at[3], dev_pair)
    dq_copy.start()
    z_up_()
    dq_copy.wait_recv()
    total_q = dqt[0] + dqrecv[...].astype(F32)
    lo, hi = total_q[0:HEAD, :].T.astype(BF16), total_q[HEAD : 2 * HEAD, :].T.astype(BF16)
    first, second = jnp.where(flips[0], hi, lo), jnp.where(flips[0], lo, hi)
    for h in range(heads):
        dq_out[0:SPAN, h * HEAD : (h + 1) * HEAD] = first[h * SPAN : (h + 1) * SPAN, :]
        dq_out[SPAN : 2 * SPAN, h * HEAD : (h + 1) * HEAD] = second[h * SPAN : (h + 1) * SPAN, :]

    total = ry_total(0)
    landed(rz.at[0], zr_r.at[2])
    landed(rz.at[1], zr_r.at[3])
    fin[...] = (total + rz[0].astype(F32) + rz[1].astype(F32)).astype(BF16)
    for o in range(1, tps):
        to = lax.rem(t + o, tps)
        to_rows = pl.ds(pl.multiple_of(to * tt, tt), tt)
        remote(fin.at[:, to_rows], kvo.at[t], a2a.at[2], a2a.at[3], (c, to)).start()
    kvo[t] = fin[:, own_rows]

    landed(kvst.at[pl.ds(0, tps - 1)], a2a.at[0])
    q_copy.wait_send()
    g_copy.wait_send()
    st_copy.wait_send()
    dq_copy.wait_send()
    half, whole = kv.at[0, 0, 0], kv.at[0, 0]
    for i in range(4):
        landed(whole if i < 2 else half, zsem_s.at[i])
        landed(half if i < 2 else whole, zr_s.at[i])
        for gi in range(NZ):
            landed(whole if i < 2 else half, ysem_s.at[gi, i])
    for gi in range(NZ):
        for i in range(2):
            landed(half, yo_s.at[gi, i])
            landed(whole, yf_s.at[gi, i])
    landed(kvo.at[pl.ds(0, tps - 1)], a2a.at[3])
    for g in range(tps):
        k_out[:, g * HEAD : (g + 1) * HEAD] = kvo[g, 0]
        v_out[:, g * HEAD : (g + 1) * HEAD] = kvo[g, 1]
    landed(kvo.at[pl.ds(0, tps - 1)], a2a.at[2])


def body(queries, keys, values, output_gradient, span_order):
    tps = lax.axis_size("tp")
    toks, width = queries.shape
    heads = width // HEAD
    rows = heads * SPAN
    tt = keys.shape[0]
    vmem = pltpu.VMEM
    half = (toks, HEAD)
    block = (2, *half)
    group = NY * SPAN
    dma = pltpu.SemaphoreType.DMA
    scratch = [
        vmem((tps, 2, tt, HEAD), BF16),
        vmem((NZ, NY, *block), BF16),
        vmem((2, heads, *half), BF16),
        vmem((2, heads, *half), BF16),
        vmem((2, rows, 2 * HEAD), BF16),
        vmem((2, rows, 2 * HEAD), BF16),
        vmem((2, 2 * HEAD, rows), BF16),
        vmem((2, 2 * HEAD, rows), BF16),
        vmem((NZ, group, HEAD), BF16),
        vmem((NZ, 2, group, 2 * HEAD), BF16),
        vmem((NZ, HEAD, group), BF16),
        vmem((NZ, 2, 2 * HEAD, group), BF16),
        vmem((NZ, group, HEAD), BF16),
        vmem((NZ, 2, group, 2 * HEAD), BF16),
        vmem((NZ, 2, 2, group, rows), F32),
        vmem((NZ, 2, 2, group, rows), F32),
        vmem((SPAN, rows), F32),
        vmem((SPAN, rows), F32),
        vmem((2, 8, rows), F32),
        vmem((2, 8, rows), F32),
        vmem((2, 8, rows), F32),
        vmem((2, 2 * HEAD, rows), F32),
        vmem((2, SPAN, HEAD), F32),
        vmem((2 * HEAD, rows), BF16),
        vmem((2 * HEAD, rows), BF16),
        vmem((NZ, NY, *block), BF16),
        vmem((NZ, *block), BF16),
        vmem((NZ, 2, *block), BF16),
        vmem(block, BF16),
        vmem((2, *block), BF16),
        vmem((3, *block), BF16),
        vmem(block, BF16),
        vmem((tps, 2, tt, HEAD), BF16),
        dma((3,)),
        dma((4,)),
        dma((4,)),
        dma((4,)),
        dma((NZ, 4)),
        dma((NZ, 4)),
        dma((4,)),
        dma((4,)),
        dma((NZ, 2)),
        dma((NZ, 2)),
        dma((NZ, 2)),
        dma((NZ, 2)),
        dma((4,)),
        dma((4,)),
    ]
    anywhere = pl.BlockSpec(memory_space=pl.ANY)
    in_vmem = pl.BlockSpec(memory_space=pltpu.VMEM)
    return tuple(
        pl.pallas_call(
            functools.partial(kernel, tps, heads),
            out_shape=(
                jax.ShapeDtypeStruct(queries.shape, BF16),
                jax.ShapeDtypeStruct(keys.shape, BF16),
                jax.ShapeDtypeStruct(values.shape, BF16),
            ),
            in_specs=[pl.BlockSpec(memory_space=pltpu.SMEM)] + [anywhere] * 4,
            out_specs=(in_vmem,) * 3,
            scratch_shapes=scratch,
            compiler_params=pltpu.CompilerParams(
                collective_id=0, has_side_effects=True, vmem_limit_bytes=56 * 1024 * 1024
            ),
        )(span_order, queries, keys, values, output_gradient)
    )


def solution(mesh):
    return jax.shard_map(
        body,
        mesh=mesh,
        in_specs=(
            P("ctx", "tp"),
            P(("ctx", "tp"), None),
            P(("ctx", "tp"), None),
            P("ctx", "tp"),
            P(),
        ),
        out_specs=(P("ctx", "tp"), P(("ctx", "tp"), None), P(("ctx", "tp"), None)),
        check_vma=False,
    )
```

```python
import functools
import math

import jax
import jax.numpy as jnp
from jax import lax
from jax.experimental import pallas as pl
from jax.experimental.pallas import tpu as pltpu
from jax.sharding import PartitionSpec as P

HEAD = 128
SPAN = 64
KV_HEADS = 8
NY = 4
NZ = 4
SCALE = HEAD**-0.5
EXPO = SCALE * math.log2(math.e)
NEG = -1e30
AG_RELAY = ()
RS_RELAY = ()
MESH = pl.DeviceIdType.MESH
F32 = jnp.float32
BF16 = jnp.bfloat16


def dot(a, b):
    return jnp.dot(a, b, preferred_element_type=F32)


def kernel(
    tps,
    heads,
    span,
    q_hbm,
    k_hbm,
    v_hbm,
    g_hbm,
    dq_out,
    k_out,
    v_out,
    kvst,
    kv,
    qs,
    gs,
    qn,
    gn,
    qt,
    gt,
    klo_s,
    kc_s,
    klot_s,
    kct_s,
    vlo_s,
    vc_s,
    s_s,
    d_s,
    s3_s,
    d3_s,
    st,
    st_in,
    cs,
    dl,
    dl_in,
    dqt,
    dk3,
    dqsend,
    dqrecv,
    out,
    ro,
    ry,
    zs,
    kvr,
    dqo,
    kvo,
    loc,
    zt_s,
    zt_r,
    ysem_s,
    ysem_r,
    pair_s,
    pair_r,
    yo_s,
    yo_r,
    yf_s,
    yf_r,
    zr_s,
    zr_r,
):
    rows = heads * SPAN
    toks = 2 * SPAN
    tt = toks // tps
    c = lax.axis_index("ctx")
    t = lax.axis_index("tp")
    core = lax.rem(c, 2)
    y = lax.rem(c // 2, NY)
    z = c // (2 * NY)

    def ctx_of(zz, yy, cc):
        return (zz * NY + yy) * 2 + cc

    y_up, y_dn, y_op = lax.rem(y + 1, NY), lax.rem(y + 3, NY), lax.rem(y + 2, NY)
    dev_yu, dev_yd = (ctx_of(z, y_up, core), t), (ctx_of(z, y_dn, core), t)
    dev_yo = (ctx_of(z, y_op, core), t)
    dev_pair = (ctx_of(z, y, 1 - core), t)

    def remote(src, dst, send, recv, device):
        return pltpu.make_async_remote_copy(
            src_ref=src,
            dst_ref=dst,
            send_sem=send,
            recv_sem=recv,
            device_id=device,
            device_id_type=MESH,
        )

    def landed(ref, sem):
        pltpu.make_async_copy(ref, ref, sem).wait()

    own_rows = pl.ds(pl.multiple_of(t * tt, tt), tt)
    own_cols = pl.ds(pl.multiple_of(t * HEAD, HEAD), HEAD)
    for w, hbm in enumerate((k_hbm, v_hbm)):
        for g in range(tps):
            pltpu.make_async_copy(
                hbm.at[:, pl.ds(g * HEAD, HEAD)], kvst.at[w, g], loc.at[w]
            ).start()
        pltpu.make_async_copy(
            hbm.at[:, own_cols], kv.at[z, y, w, own_rows], zt_r.at[w, z]
        ).start()
    for h in range(heads):
        cols = pl.ds(h * HEAD, HEAD)
        pltpu.make_async_copy(q_hbm.at[:, cols], qs.at[0, h], loc.at[2]).start()
        pltpu.make_async_copy(g_hbm.at[:, cols], gs.at[0, h], loc.at[3]).start()

    def z_of(gi):
        return lax.rem(z + gi + (gi // 2) * (1 - 2 * (gi % 2)), NZ)

    def greet(device):
        pl.semaphore_signal(barrier, inc=1, device_id=device, device_id_type=MESH)

    barrier = pltpu.get_barrier_semaphore()
    for gi in range(NZ):
        for o in range(1 if gi == 0 else 0, tps):
            greet((ctx_of(z_of(gi), y, core), lax.rem(t + o, tps)))
    for device in (dev_yu, dev_yd, dev_yo, dev_pair):
        greet(device)
    landed(kvst.at[0], loc.at[0])
    landed(kvst.at[1], loc.at[1])
    pl.semaphore_wait(barrier, NZ * tps - 1 + 4)

    for w, gi in ((0, 0), (1, 0), (0, 1), (0, 2), (0, 3), (1, 1), (1, 2), (1, 3)):
        for o in range(1 if gi == 0 else 0, tps):
            to = lax.rem(t + o, tps)
            device = (ctx_of(z_of(gi), y, core), to)
            remote(
                kvst.at[w, to], kv.at[z, y, w, own_rows], zt_s.at[w, gi], zt_r.at[w, z], device
            ).start()
    landed(qs.at[0], loc.at[2])
    q_copy = remote(qs.at[0], qs.at[1], pair_s.at[0], pair_r.at[0], dev_pair)
    q_copy.start()
    landed(gs.at[0], loc.at[3])
    g_copy = remote(gs.at[0], gs.at[1], pair_s.at[1], pair_r.at[1], dev_pair)
    g_copy.start()

    def spans(cc):
        s0, s1 = span[2 * cc], span[2 * cc + 1]
        return s0 > s1, jnp.minimum(s0, s1)

    devs = (c, ctx_of(z, y, 1 - core))
    flips, lows = zip(*[spans(d) for d in devs])

    def prepare(a, src, normal, turned):
        first = src[a, :, 0:SPAN, :].reshape(rows, HEAD)
        second = src[a, :, SPAN : 2 * SPAN, :].reshape(rows, HEAD)
        lo = jnp.where(flips[a], second, first)
        hi = jnp.where(flips[a], first, second)
        normal[a, :, 0:HEAD] = lo
        normal[a, :, HEAD : 2 * HEAD] = hi
        turned[a, 0:HEAD, :] = lo.T
        turned[a, HEAD : 2 * HEAD, :] = hi.T

    low, high = pl.ds(0, SPAN), pl.ds(SPAN, SPAN)

    def y_send(w, gi):
        zg = z_of(gi)
        b = kv.at[zg, y, w]
        landed(b, zt_r.at[w, zg])
        remote(b, b, ysem_s.at[w, gi, 0], ysem_r.at[w, gi, 0], dev_yu).start()
        remote(b, b, ysem_s.at[w, gi, 1], ysem_r.at[w, gi, 1], dev_yd).start()
        if (w, gi) not in AG_RELAY:
            remote(b, b, ysem_s.at[w, gi, 2], ysem_r.at[w, gi, 2], dev_yo).start()

    def y_relay(w, gi):
        zg = z_of(gi)
        landed(kv.at[zg, y_dn, w], ysem_r.at[w, gi, 0])
        b = kv.at[zg, y_dn, w, low]
        remote(b, b, ysem_s.at[w, gi, 2], ysem_r.at[w, gi, 2], dev_yu).start()
        landed(kv.at[zg, y_up, w], ysem_r.at[w, gi, 1])
        b = kv.at[zg, y_up, w, high]
        remote(b, b, ysem_s.at[w, gi, 3], ysem_r.at[w, gi, 3], dev_yd).start()

    def y_done(w, gi):
        zg = z_of(gi)
        if (w, gi) in AG_RELAY:
            landed(kv.at[zg, y_op, w, low], ysem_r.at[w, gi, 2])
            landed(kv.at[zg, y_op, w, high], ysem_r.at[w, gi, 3])
        else:
            landed(kv.at[zg, y_dn, w], ysem_r.at[w, gi, 0])
            landed(kv.at[zg, y_up, w], ysem_r.at[w, gi, 1])
            landed(kv.at[zg, y_op, w], ysem_r.at[w, gi, 2])

    def at(gi, todo):
        for g in range(NZ):
            pl.when(gi == g)(functools.partial(todo, g))

    y_send(0, 0)
    prepare(0, qs, qn, qt)
    y_send(0, 1)
    y_send(0, 2)

    def lohi(zg, yy, w):
        first, second = kv[zg, yy, w, 0:SPAN, :], kv[zg, yy, w, SPAN : 2 * SPAN, :]
        flip, _ = spans(ctx_of(zg, yy, core))
        return jnp.where(flip, second, first), jnp.where(flip, first, second)

    key_i = lax.broadcasted_iota(jnp.int32, (SPAN, rows), 0)
    tok_i = lax.rem(lax.broadcasted_iota(jnp.int32, (SPAN, rows), 1), SPAN)
    hidden = key_i > tok_i

    s3 = jnp.where(hidden, NEG, dot(lohi(z, y, 0)[0], qt[0, 0:HEAD, :]))
    s3_s[...] = s3
    m3 = jnp.max(s3, axis=0, keepdims=True)
    e3 = jnp.exp2((s3 - m3) * EXPO)
    none = jnp.full((1, rows), NEG, F32)
    zero = jnp.zeros((1, rows), F32)
    for a in range(2):
        st[a, 0:1, :] = none if a else m3
        st[a, 1:2, :] = zero if a else jnp.sum(e3, axis=0, keepdims=True)
        st[a, 2:3, :] = none
        st[a, 3:8, :] = jnp.zeros((5, rows), F32)
    y_send(0, 3)
    y_send(1, 0)
    prepare(0, gs, gn, gt)
    d3_s[...] = dot(lohi(z, y, 1)[0], gt[0, 0:HEAD, :])
    q_copy.wait_recv()
    prepare(1, qs, qn, qt)
    y_send(1, 1)
    y_send(1, 2)
    y_send(1, 3)

    def picks(zg, a):
        return [spans(ctx_of(zg, yy, core))[1] < lows[a] for yy in range(NY)]

    def block(yy):
        return slice(yy * SPAN, (yy + 1) * SPAN)

    def split(zg, w, lo_s, cat_s, gi):
        pairs = [lohi(zg, yy, w) for yy in range(NY)]
        for yy in range(NY):
            lo_s[gi, block(yy), :] = pairs[yy][0]
        for a in range(2):
            pick = picks(zg, a)
            for yy in range(NY):
                lo, hi = pairs[yy]
                none_ = jnp.zeros_like(lo)
                cat_s[gi, a, block(yy), 0:HEAD] = jnp.where(pick[yy], lo, none_)
                cat_s[gi, a, block(yy), HEAD : 2 * HEAD] = jnp.where(pick[yy], none_, hi)

    def column_sum(x):
        return jnp.sum(x, axis=0, keepdims=True)

    def scores(gi):
        zg = z_of(gi)
        split(zg, 0, klo_s, kc_s, gi)
        for a in range(2):
            pick = picks(zg, a)
            s1 = dot(klo_s[gi], qt[a, HEAD : 2 * HEAD, :])
            s2 = dot(kc_s[gi, a], qt[a])
            s_s[gi, a, 0] = s1
            parts = []
            for yy in range(NY):
                part = s2[block(yy), :]
                if a == 0:
                    here = jnp.logical_and(zg == z, yy == y)
                    part = jnp.where(jnp.logical_and(hidden, here), NEG, part)
                s_s[gi, a, 1, block(yy), :] = part
                parts.append(part)
            m_lo, l_lo, m_hi, l_hi = (st[a, i : i + 1, :] for i in range(4))
            n_lo, n_hi = m_lo, jnp.maximum(m_hi, jnp.max(s1, axis=0, keepdims=True))
            for yy in range(NY):
                top = jnp.max(parts[yy], axis=0, keepdims=True)
                n_lo = jnp.maximum(n_lo, jnp.where(pick[yy], top, none))
                n_hi = jnp.maximum(n_hi, jnp.where(pick[yy], none, top))
            l_lo = l_lo * jnp.exp2((m_lo - n_lo) * EXPO)
            l_hi = l_hi * jnp.exp2((m_hi - n_hi) * EXPO)
            l_hi = l_hi + column_sum(jnp.exp2((s1 - n_hi) * EXPO))
            for yy in range(NY):
                e2 = jnp.exp2((parts[yy] - jnp.where(pick[yy], n_lo, n_hi)) * EXPO)
                total = column_sum(e2)
                l_lo = l_lo + jnp.where(pick[yy], total, zero)
                l_hi = l_hi + jnp.where(pick[yy], zero, total)
            for i, x in enumerate((n_lo, l_lo, n_hi, l_hi)):
                st[a, i : i + 1, :] = x

    def score_step(gi, carry):
        at(gi, functools.partial(y_done, 0))
        scores(gi)
        return carry

    lax.fori_loop(0, NZ, score_step, 0)

    st_copy = remote(st, st_in, pair_s.at[2], pair_r.at[2], dev_pair)
    st_copy.start()
    dqt[...] = jnp.zeros_like(dqt)
    g_copy.wait_recv()
    prepare(1, gs, gn, gt)
    st_copy.wait_recv()
    for a in range(2):
        for at_ in (0, 2):
            m0, l0 = (st[a, at_ + i : at_ + i + 1, :] for i in range(2))
            m1, l1 = (st_in[1 - a, at_ + i : at_ + i + 1, :] for i in range(2))
            m = jnp.maximum(m0, m1)
            total = l0 * jnp.exp2((m0 - m) * EXPO) + l1 * jnp.exp2((m1 - m) * EXPO)
            cs[a, at_ : at_ + 1, :] = m
            cs[a, at_ + 1 : at_ + 2, :] = 1.0 / total

    def prob_of(s, m, inv):
        return jnp.exp2((s - m) * EXPO) * inv

    p3 = prob_of(s3_s[...], cs[0, 0:1, :], cs[0, 1:2, :])
    s3_s[...] = p3
    dk3[1] = dot(p3.astype(BF16), gn[0, :, 0:HEAD])
    for a in range(2):
        dl[a, 0:1, :] = zero if a else column_sum(p3 * d3_s[...])
        dl[a, 1:8, :] = jnp.zeros((7, rows), F32)

    def collect(gi, w, tiles, wide):
        zg = z_of(gi)
        dlo, dhi = [None] * NY, [None] * NY
        for a in range(2):
            x1, x2 = tiles(a)
            pick = picks(zg, a)
            one = dot(x1, wide[a, :, HEAD : 2 * HEAD])
            two = dot(x2, wide[a])
            for yy in range(NY):
                left, right = two[block(yy), 0:HEAD], two[block(yy), HEAD : 2 * HEAD]
                none_ = jnp.zeros_like(left)
                new_lo = one[block(yy), :] + jnp.where(pick[yy], left, none_)
                new_hi = jnp.where(pick[yy], none_, right)
                if a == 0:
                    here = jnp.logical_and(zg == z, yy == y)
                    dlo[yy], dhi[yy] = new_lo + jnp.where(here, dk3[w], none_), new_hi
                else:
                    dlo[yy], dhi[yy] = dlo[yy] + new_lo, dhi[yy] + new_hi
        for yy in range(NY):
            flip, _ = spans(ctx_of(zg, yy, core))
            out[zg, yy, w, 0:SPAN, :] = jnp.where(flip, dhi[yy], dlo[yy]).astype(BF16)
            out[zg, yy, w, SPAN : 2 * SPAN, :] = jnp.where(flip, dlo[yy], dhi[yy]).astype(BF16)

    def value_grads(gi):
        zg = z_of(gi)
        split(zg, 1, vlo_s, vc_s, gi)

        def tiles(a):
            pick = picks(zg, a)
            m_lo, i_lo, m_hi, i_hi = (cs[a, i : i + 1, :] for i in range(4))
            d1 = dot(vlo_s[gi], gt[a, HEAD : 2 * HEAD, :])
            d2 = dot(vc_s[gi, a], gt[a])
            d_s[gi, a, 0] = d1
            d_s[gi, a, 1] = d2
            p1 = prob_of(s_s[gi, a, 0], m_hi, i_hi)
            s_s[gi, a, 0] = p1
            e_lo, e_hi = dl[a, 0:1, :], dl[a, 1:2, :] + column_sum(p1 * d1)
            w2 = []
            for yy in range(NY):
                p2 = prob_of(
                    s_s[gi, a, 1, block(yy), :],
                    jnp.where(pick[yy], m_lo, m_hi),
                    jnp.where(pick[yy], i_lo, i_hi),
                )
                s_s[gi, a, 1, block(yy), :] = p2
                inner = column_sum(p2 * d2[block(yy), :])
                e_lo = e_lo + jnp.where(pick[yy], inner, zero)
                e_hi = e_hi + jnp.where(pick[yy], zero, inner)
                w2.append(p2.astype(BF16))
            dl[a, 0:1, :] = e_lo
            dl[a, 1:2, :] = e_hi
            return p1.astype(BF16), jnp.concatenate(w2, axis=0)

        collect(gi, 1, tiles, gn)
        klot_s[gi] = klo_s[gi].T
        for a in range(2):
            kct_s[gi, a] = kc_s[gi, a].T

    def score_grad(p, d, delta):
        return (p * (d - delta) * SCALE).astype(BF16)

    def key_grads(gi):
        zg = z_of(gi)

        def tiles(a):
            pick = picks(zg, a)
            e_lo, e_hi = (dl[a, i : i + 1, :] + dl_in[1 - a, i : i + 1, :] for i in range(2))
            ds1 = score_grad(s_s[gi, a, 0], d_s[gi, a, 0], e_hi)
            ds2 = jnp.concatenate(
                [
                    score_grad(
                        s_s[gi, a, 1, block(yy), :],
                        d_s[gi, a, 1, block(yy), :],
                        jnp.where(pick[yy], e_lo, e_hi),
                    )
                    for yy in range(NY)
                ],
                axis=0,
            )
            dqt[a] += dot(kct_s[gi, a], ds2)
            dqt[a, HEAD : 2 * HEAD, :] += dot(klot_s[gi], ds1)
            return ds1, ds2

        collect(gi, 0, tiles, qn)

    def plus(a, b):
        return (a.astype(F32) + b.astype(F32)).astype(BF16)

    def ry_first(w, gi):
        zg = z_of(gi)
        if (w, gi) in RS_RELAY:
            remote(
                out.at[zg, y_op, w, low], ro.at[gi, w, low], yo_s.at[w, gi, 0], yo_r.at[w, gi, 0], dev_yu
            ).start()
            remote(
                out.at[zg, y_op, w, high], ro.at[gi, w, high], yo_s.at[w, gi, 1], yo_r.at[w, gi, 1], dev_yd
            ).start()
        else:
            ry_near(w, gi, 0)
            ry_near(w, gi, 1)
            remote(
                out.at[zg, y_op, w], ro.at[gi, w], yo_s.at[w, gi, 0], yo_r.at[w, gi, 0], dev_yo
            ).start()

    def ry_near(w, gi, i):
        b = out.at[z_of(gi), (y_up, y_dn)[i], w]
        remote(
            b, ry.at[gi, i, w], yf_s.at[w, gi, i], yf_r.at[w, gi, i], (dev_yu, dev_yd)[i]
        ).start()

    def ry_forward(w, gi):
        zg = z_of(gi)
        landed(ro.at[gi, w, low], yo_r.at[w, gi, 0])
        out[zg, y_up, w, low] = plus(out[zg, y_up, w, low], ro[gi, w, low])
        ry_near(w, gi, 0)
        landed(ro.at[gi, w, high], yo_r.at[w, gi, 1])
        out[zg, y_dn, w, high] = plus(out[zg, y_dn, w, high], ro[gi, w, high])
        ry_near(w, gi, 1)

    def ry_total(w, gi):
        zg = z_of(gi)
        landed(ry.at[gi, 0, w], yf_r.at[w, gi, 0])
        landed(ry.at[gi, 1, w], yf_r.at[w, gi, 1])
        total = out[zg, y, w].astype(F32) + ry[gi, 0, w].astype(F32) + ry[gi, 1, w].astype(F32)
        if (w, gi) not in RS_RELAY:
            landed(ro.at[gi, w], yo_r.at[w, gi, 0])
            total = total + ro[gi, w].astype(F32)
        zs[gi, w] = total.astype(BF16)
        for o in range(1 if gi == 0 else 0, tps):
            to = lax.rem(t + o, tps)
            to_rows = pl.ds(pl.multiple_of(to * tt, tt), tt)
            device = (ctx_of(zg, y, core), to)
            remote(
                zs.at[gi, w, to_rows], kvr.at[z, w, t], zr_s.at[w, gi], zr_r.at[w, z], device
            ).start()

    def value_step(gi, carry):
        at(gi, functools.partial(y_done, 1))
        value_grads(gi)
        at(gi, functools.partial(ry_first, 1))
        return carry

    lax.fori_loop(0, NZ, value_step, 0)

    dl_copy = remote(dl, dl_in, pair_s.at[4], pair_r.at[4], dev_pair)
    dl_copy.start()
    dl_copy.wait_recv()
    ds3 = score_grad(s3_s[...], d3_s[...], dl[0, 0:1, :] + dl_in[1, 0:1, :])
    dk3[0] = dot(ds3, qn[0, :, 0:HEAD])
    dqt[0, 0:HEAD, :] = dot(lohi(z, y, 0)[0].T, ds3)

    def key_step(i, carry):
        gi = NZ - 1 - i
        key_grads(gi)
        at(gi, functools.partial(ry_first, 0))
        return carry

    lax.fori_loop(0, NZ, key_step, 0)

    dqsend[...] = dqt[1].astype(BF16)
    for gi in range(NZ - 1, -1, -1):
        ry_total(1, gi)
    dq_copy = remote(dqsend, dqrecv, pair_s.at[3], pair_r.at[3], dev_pair)
    dq_copy.start()
    kvr[z, 1, t] = zs[0, 1, own_rows]
    ry_total(0, 3)
    dq_copy.wait_recv()
    total_q = dqt[0] + dqrecv[...].astype(F32)
    lo, hi = total_q[0:HEAD, :].T.astype(BF16), total_q[HEAD : 2 * HEAD, :].T.astype(BF16)
    first, second = jnp.where(flips[0], hi, lo), jnp.where(flips[0], lo, hi)
    for h in range(heads):
        dqo[0:SPAN, h * HEAD : (h + 1) * HEAD] = first[h * SPAN : (h + 1) * SPAN, :]
        dqo[SPAN : 2 * SPAN, h * HEAD : (h + 1) * HEAD] = second[h * SPAN : (h + 1) * SPAN, :]
    ry_total(0, 2)
    results = [pltpu.make_async_copy(dqo, dq_out, loc.at[0])]
    results[0].start()
    ry_total(0, 1)
    ry_total(0, 0)
    kvr[z, 0, t] = zs[0, 0, own_rows]

    for copy in (q_copy, g_copy, st_copy, dl_copy, dq_copy):
        copy.wait_send()
    whole = kv.at[0, 0, 0]
    half = kv.at[0, 0, 0, low]
    pieces = [kvst.at[0, pl.ds(0, tps - 1)]] + [kvst.at[0]] * (NZ - 1)
    for w in range(2):
        for gi in range(NZ):
            landed(pieces[gi], zt_s.at[w, gi])
            landed(pieces[gi], zr_s.at[w, gi])
            relay = (w, gi) in AG_RELAY
            for i in range(4 if relay else 3):
                landed(half if relay and i >= 2 else whole, ysem_s.at[w, gi, i])
            relay = (w, gi) in RS_RELAY
            for i in range(2 if relay else 1):
                landed(half if relay else whole, yo_s.at[w, gi, i])
            for i in range(2):
                landed(whole, yf_s.at[w, gi, i])
    for w, result in ((1, v_out), (0, k_out)):
        for gi in range(NZ - 1, -1, -1):
            landed(pieces[gi], zr_r.at[w, z_of(gi)])
        for g in range(tps):
            total = kvr[0, w, g].astype(F32)
            for i in range(1, NZ):
                total = total + kvr[i, w, g].astype(F32)
            kvo[w, :, g * HEAD : (g + 1) * HEAD] = total.astype(BF16)
        results.append(pltpu.make_async_copy(kvo.at[w], result, loc.at[1 + w]))
        results[-1].start()
    for copy in results:
        copy.wait()


def body(queries, keys, values, output_gradient, span_order):
    tps = lax.axis_size("tp")
    toks, width = queries.shape
    heads = width // HEAD
    rows = heads * SPAN
    tt = keys.shape[0]
    vmem = pltpu.VMEM
    half = (toks, HEAD)
    block = (2, *half)
    group = NY * SPAN
    dma = pltpu.SemaphoreType.DMA
    scratch = [
        vmem((2, tps, tt, HEAD), BF16),
        vmem((NZ, NY, *block), BF16),
        vmem((2, heads, *half), BF16),
        vmem((2, heads, *half), BF16),
        vmem((2, rows, 2 * HEAD), BF16),
        vmem((2, rows, 2 * HEAD), BF16),
        vmem((2, 2 * HEAD, rows), BF16),
        vmem((2, 2 * HEAD, rows), BF16),
        vmem((NZ, group, HEAD), BF16),
        vmem((NZ, 2, group, 2 * HEAD), BF16),
        vmem((NZ, HEAD, group), BF16),
        vmem((NZ, 2, 2 * HEAD, group), BF16),
        vmem((NZ, group, HEAD), BF16),
        vmem((NZ, 2, group, 2 * HEAD), BF16),
        vmem((NZ, 2, 2, group, rows), F32),
        vmem((NZ, 2, 2, group, rows), F32),
        vmem((SPAN, rows), F32),
        vmem((SPAN, rows), F32),
        vmem((2, 8, rows), F32),
        vmem((2, 8, rows), F32),
        vmem((2, 8, rows), F32),
        vmem((2, 8, rows), F32),
        vmem((2, 8, rows), F32),
        vmem((2, 2 * HEAD, rows), F32),
        vmem((2, SPAN, HEAD), F32),
        vmem((2 * HEAD, rows), BF16),
        vmem((2 * HEAD, rows), BF16),
        vmem((NZ, NY, *block), BF16),
        vmem((NZ, *block), BF16),
        vmem((NZ, 2, *block), BF16),
        vmem((NZ, *block), BF16),
        vmem((NZ, 2, tps, tt, HEAD), BF16),
        vmem(queries.shape, BF16),
        vmem((2, *keys.shape), BF16),
        dma((4,)),
        dma((2, NZ)),
        dma((2, NZ)),
        dma((2, NZ, 4)),
        dma((2, NZ, 4)),
        dma((5,)),
        dma((5,)),
        dma((2, NZ, 2)),
        dma((2, NZ, 2)),
        dma((2, NZ, 2)),
        dma((2, NZ, 2)),
        dma((2, NZ)),
        dma((2, NZ)),
    ]
    anywhere = pl.BlockSpec(memory_space=pl.ANY)
    return tuple(
        pl.pallas_call(
            functools.partial(kernel, tps, heads),
            out_shape=(
                jax.ShapeDtypeStruct(queries.shape, BF16),
                jax.ShapeDtypeStruct(keys.shape, BF16),
                jax.ShapeDtypeStruct(values.shape, BF16),
            ),
            in_specs=[pl.BlockSpec(memory_space=pltpu.SMEM)] + [anywhere] * 4,
            out_specs=(anywhere,) * 3,
            scratch_shapes=scratch,
            compiler_params=pltpu.CompilerParams(
                collective_id=0, has_side_effects=True, vmem_limit_bytes=56 * 1024 * 1024
            ),
        )(span_order, queries, keys, values, output_gradient)
    )


def solution(mesh):
    return jax.shard_map(
        body,
        mesh=mesh,
        in_specs=(
            P("ctx", "tp"),
            P(("ctx", "tp"), None),
            P(("ctx", "tp"), None),
            P("ctx", "tp"),
            P(),
        ),
        out_specs=(P("ctx", "tp"), P(("ctx", "tp"), None), P(("ctx", "tp"), None)),
        check_vma=False,
    )
```

```python
import functools
import math

import jax
import jax.numpy as jnp
from jax import lax
from jax.experimental import pallas as pl
from jax.experimental.pallas import tpu as pltpu
from jax.sharding import PartitionSpec as P

HEAD = 128
SPAN = 64
KV_HEADS = 8
NY = 4
NZ = 4
SCALE = HEAD**-0.5
EXPO = SCALE * math.log2(math.e)
NEG = -1e30
ZT_FIRST = ((0, 0), (1, 0), (0, 1), (0, 2), (0, 3), (1, 1), (1, 2), (1, 3))
AG_RELAY = ()
INNER_AHEAD = 1
Z_FIRST = ()
RS_RELAY = ()
POINTS = {'first': (('send', 1, 0),), 'second': (), 'third': (), 'score': {0: (('send', 1, 1),), 1: (('send', 1, 2),), 2: (('send', 1, 3),)}, 'stats': (('inner', 1, 0),), 'delta': (), 'key': {2: (('total', 1, 1),), 3: (('total', 1, 2),)}, 'keys': (), 'last': (('total', 1, 3), ('total', 1, 0), ('total', 0, 3), ('total', 0, 2)), 'end': (('total', 0, 1), ('total', 0, 0)), 'value': {}}
MESH = pl.DeviceIdType.MESH
F32 = jnp.float32
BF16 = jnp.bfloat16


def dot(a, b):
    return jnp.dot(a, b, preferred_element_type=F32)


def kernel(
    tps,
    heads,
    span,
    q_hbm,
    k_hbm,
    v_hbm,
    g_hbm,
    dq_out,
    k_out,
    v_out,
    kvst,
    kv,
    qs,
    gs,
    qn,
    gn,
    qt,
    gt,
    klo_s,
    kc_s,
    vlo_s,
    vc_s,
    s_s,
    d_s,
    ds_s,
    s3_s,
    d3_s,
    st,
    st_in,
    cs,
    dl,
    dl_in,
    dqt,
    dk3,
    dqsend,
    dqrecv,
    out,
    ro,
    ry,
    zs,
    kvr,
    rzv,
    loc,
    zt_s,
    zt_r,
    ysem_s,
    ysem_r,
    pair_s,
    pair_r,
    yo_s,
    yo_r,
    yf_s,
    yf_r,
    zr_s,
    zr_r,
    zv_s,
    zv_r,
):
    rows = heads * SPAN
    toks = 2 * SPAN
    tt = toks // tps
    c = lax.axis_index("ctx")
    t = lax.axis_index("tp")
    core = lax.rem(c, 2)
    y = lax.rem(c // 2, NY)
    z = c // (2 * NY)

    def ctx_of(zz, yy, cc):
        return (zz * NY + yy) * 2 + cc

    y_up, y_dn, y_op = lax.rem(y + 1, NY), lax.rem(y + 3, NY), lax.rem(y + 2, NY)
    dev_yu, dev_yd = (ctx_of(z, y_up, core), t), (ctx_of(z, y_dn, core), t)
    dev_yo = (ctx_of(z, y_op, core), t)
    dev_pair = (ctx_of(z, y, 1 - core), t)

    def remote(src, dst, send, recv, device):
        return pltpu.make_async_remote_copy(
            src_ref=src,
            dst_ref=dst,
            send_sem=send,
            recv_sem=recv,
            device_id=device,
            device_id_type=MESH,
        )

    def landed(ref, sem):
        pltpu.make_async_copy(ref, ref, sem).wait()

    own_rows = pl.ds(pl.multiple_of(t * tt, tt), tt)
    own_cols = pl.ds(pl.multiple_of(t * HEAD, HEAD), HEAD)

    def fetch(w, hbm):
        for g in range(tps):
            pltpu.make_async_copy(
                hbm.at[:, pl.ds(g * HEAD, HEAD)], kvst.at[w, g], loc.at[w]
            ).start()
        pltpu.make_async_copy(
            hbm.at[:, own_cols], kv.at[z, y, w, own_rows], zt_r.at[w, z]
        ).start()

    fetch(0, k_hbm)

    def z_of(gi):
        return lax.rem(z + gi + (gi // 2) * (1 - 2 * (gi % 2)), NZ)

    def greet(device):
        pl.semaphore_signal(barrier, inc=1, device_id=device, device_id_type=MESH)

    barrier = pltpu.get_barrier_semaphore()
    for gi in range(NZ):
        for o in range(1 if gi == 0 else 0, tps):
            greet((ctx_of(z_of(gi), y, core), lax.rem(t + o, tps)))
    for device in (dev_yu, dev_yd, dev_yo, dev_pair):
        greet(device)
    fetch(1, v_hbm)
    landed(kvst.at[0], loc.at[0])
    landed(kvst.at[1], loc.at[1])
    pl.semaphore_wait(barrier, NZ * tps - 1 + 4)

    def zt_send(w, gi):
        for o in range(1 if gi == 0 else 0, tps):
            to = lax.rem(t + o, tps)
            device = (ctx_of(z_of(gi), y, core), to)
            remote(
                kvst.at[w, to], kv.at[z, y, w, own_rows], zt_s.at[w, gi], zt_r.at[w, z], device
            ).start()

    for w, gi in ZT_FIRST:
        zt_send(w, gi)
    for h in range(heads):
        cols = pl.ds(h * HEAD, HEAD)
        pltpu.make_async_copy(q_hbm.at[:, cols], qs.at[0, h], loc.at[2]).start()
        pltpu.make_async_copy(g_hbm.at[:, cols], gs.at[0, h], loc.at[3]).start()
    landed(qs.at[0], loc.at[2])
    q_copy = remote(qs.at[0], qs.at[1], pair_s.at[0], pair_r.at[0], dev_pair)
    q_copy.start()
    landed(gs.at[0], loc.at[3])
    g_copy = remote(gs.at[0], gs.at[1], pair_s.at[1], pair_r.at[1], dev_pair)
    g_copy.start()

    def spans(cc):
        s0, s1 = span[2 * cc], span[2 * cc + 1]
        return s0 > s1, jnp.minimum(s0, s1)

    devs = (c, ctx_of(z, y, 1 - core))
    flips, lows = zip(*[spans(d) for d in devs])

    def prepare(a, src, normal, turned):
        first = src[a, :, 0:SPAN, :].reshape(rows, HEAD)
        second = src[a, :, SPAN : 2 * SPAN, :].reshape(rows, HEAD)
        lo = jnp.where(flips[a], second, first)
        hi = jnp.where(flips[a], first, second)
        normal[a, :, 0:HEAD] = lo
        normal[a, :, HEAD : 2 * HEAD] = hi
        turned[a, 0:HEAD, :] = lo.T
        turned[a, HEAD : 2 * HEAD, :] = hi.T

    low, high = pl.ds(0, SPAN), pl.ds(SPAN, SPAN)

    def y_send(w, gi):
        zg = z_of(gi)
        b = kv.at[zg, y, w]
        landed(b, zt_r.at[w, zg])
        remote(b, b, ysem_s.at[w, gi, 0], ysem_r.at[w, gi, 0], dev_yu).start()
        remote(b, b, ysem_s.at[w, gi, 1], ysem_r.at[w, gi, 1], dev_yd).start()
        if (w, gi) not in AG_RELAY:
            remote(b, b, ysem_s.at[w, gi, 2], ysem_r.at[w, gi, 2], dev_yo).start()

    def y_relay(w, gi):
        zg = z_of(gi)
        landed(kv.at[zg, y_dn, w], ysem_r.at[w, gi, 0])
        b = kv.at[zg, y_dn, w, low]
        remote(b, b, ysem_s.at[w, gi, 2], ysem_r.at[w, gi, 2], dev_yu).start()
        landed(kv.at[zg, y_up, w], ysem_r.at[w, gi, 1])
        b = kv.at[zg, y_up, w, high]
        remote(b, b, ysem_s.at[w, gi, 3], ysem_r.at[w, gi, 3], dev_yd).start()

    def y_done(w, gi):
        zg = z_of(gi)
        if (w, gi) in AG_RELAY:
            landed(kv.at[zg, y_op, w, low], ysem_r.at[w, gi, 2])
            landed(kv.at[zg, y_op, w, high], ysem_r.at[w, gi, 3])
        else:
            landed(kv.at[zg, y_dn, w], ysem_r.at[w, gi, 0])
            landed(kv.at[zg, y_up, w], ysem_r.at[w, gi, 1])
            landed(kv.at[zg, y_op, w], ysem_r.at[w, gi, 2])

    steps = {}

    def act(name, g=None):
        for step, w, gi in POINTS[name] if g is None else POINTS[name].get(g, ()):
            steps[step](w, gi)

    def point(name, i):
        for g in POINTS[name]:
            pl.when(i == g)(functools.partial(act, name, g))

    def at(gi, todo):
        for g in range(NZ):
            pl.when(gi == g)(functools.partial(todo, g))

    steps["relay"], steps["send"] = y_relay, y_send
    y_send(0, 0)
    prepare(0, qs, qn, qt)
    steps["zt"] = zt_send
    act("first")
    y_send(0, 1)
    y_send(0, 2)
    act("second")

    def lohi(zg, yy, w):
        first, second = kv[zg, yy, w, 0:SPAN, :], kv[zg, yy, w, SPAN : 2 * SPAN, :]
        flip, _ = spans(ctx_of(zg, yy, core))
        return jnp.where(flip, second, first), jnp.where(flip, first, second)

    key_i = lax.broadcasted_iota(jnp.int32, (SPAN, rows), 0)
    tok_i = lax.rem(lax.broadcasted_iota(jnp.int32, (SPAN, rows), 1), SPAN)
    hidden = key_i > tok_i

    s3 = jnp.where(hidden, NEG, dot(lohi(z, y, 0)[0], qt[0, 0:HEAD, :]))
    s3_s[...] = s3
    m3 = jnp.max(s3, axis=0, keepdims=True)
    e3 = jnp.exp2((s3 - m3) * EXPO)
    none = jnp.full((1, rows), NEG, F32)
    zero = jnp.zeros((1, rows), F32)
    for a in range(2):
        st[a, 0:1, :] = none if a else m3
        st[a, 1:2, :] = zero if a else jnp.sum(e3, axis=0, keepdims=True)
        st[a, 2:3, :] = none
        st[a, 3:8, :] = jnp.zeros((5, rows), F32)
    y_send(0, 3)
    act("third")
    prepare(0, gs, gn, gt)
    q_copy.wait_recv()
    prepare(1, qs, qn, qt)
    def picks(zg, a):
        return [spans(ctx_of(zg, yy, core))[1] < lows[a] for yy in range(NY)]

    def block(yy):
        return slice(yy * SPAN, (yy + 1) * SPAN)

    def split(zg, w, lo_s, cat_s, gi):
        pairs = [lohi(zg, yy, w) for yy in range(NY)]
        for yy in range(NY):
            lo_s[gi, block(yy), :] = pairs[yy][0]
        for a in range(2):
            pick = picks(zg, a)
            for yy in range(NY):
                lo, hi = pairs[yy]
                none_ = jnp.zeros_like(lo)
                cat_s[gi, a, block(yy), 0:HEAD] = jnp.where(pick[yy], lo, none_)
                cat_s[gi, a, block(yy), HEAD : 2 * HEAD] = jnp.where(pick[yy], none_, hi)

    def column_sum(x):
        return jnp.sum(x, axis=0, keepdims=True)

    def scores(gi):
        zg = z_of(gi)
        split(zg, 0, klo_s, kc_s, gi)
        for a in range(2):
            pick = picks(zg, a)
            s1 = dot(klo_s[gi], qt[a, HEAD : 2 * HEAD, :])
            s2 = dot(kc_s[gi, a], qt[a])
            s_s[gi, a, 0] = s1
            parts = []
            for yy in range(NY):
                part = s2[block(yy), :]
                if a == 0:
                    here = jnp.logical_and(zg == z, yy == y)
                    part = jnp.where(jnp.logical_and(hidden, here), NEG, part)
                s_s[gi, a, 1, block(yy), :] = part
                parts.append(part)
            m_lo, l_lo, m_hi, l_hi = (st[a, i : i + 1, :] for i in range(4))
            n_lo, n_hi = m_lo, jnp.maximum(m_hi, jnp.max(s1, axis=0, keepdims=True))
            for yy in range(NY):
                top = jnp.max(parts[yy], axis=0, keepdims=True)
                n_lo = jnp.maximum(n_lo, jnp.where(pick[yy], top, none))
                n_hi = jnp.maximum(n_hi, jnp.where(pick[yy], none, top))
            l_lo = l_lo * jnp.exp2((m_lo - n_lo) * EXPO)
            l_hi = l_hi * jnp.exp2((m_hi - n_hi) * EXPO)
            l_hi = l_hi + column_sum(jnp.exp2((s1 - n_hi) * EXPO))
            for yy in range(NY):
                e2 = jnp.exp2((parts[yy] - jnp.where(pick[yy], n_lo, n_hi)) * EXPO)
                total = column_sum(e2)
                l_lo = l_lo + jnp.where(pick[yy], total, zero)
                l_hi = l_hi + jnp.where(pick[yy], zero, total)
            for i, x in enumerate((n_lo, l_lo, n_hi, l_hi)):
                st[a, i : i + 1, :] = x

    def inner(gi):
        split(z_of(gi), 1, vlo_s, vc_s, gi)
        for a in range(2):
            d_s[gi, a, 0] = dot(vlo_s[gi], gt[a, HEAD : 2 * HEAD, :])
            d_s[gi, a, 1] = dot(vc_s[gi, a], gt[a])

    def inner_now(w, gi):
        y_done(w, gi)
        inner(gi)

    steps["inner"] = inner_now

    def score_step(gi, carry):
        at(gi, functools.partial(y_done, 0))
        scores(gi)
        point("score", gi)
        return carry

    lax.fori_loop(0, NZ, score_step, 0)

    st_copy = remote(st, st_in, pair_s.at[2], pair_r.at[2], dev_pair)
    st_copy.start()
    dqt[...] = jnp.zeros_like(dqt)
    g_copy.wait_recv()
    prepare(1, gs, gn, gt)
    act("stats")
    st_copy.wait_recv()
    for a in range(2):
        for at_ in (0, 2):
            m0, l0 = (st[a, at_ + i : at_ + i + 1, :] for i in range(2))
            m1, l1 = (st_in[1 - a, at_ + i : at_ + i + 1, :] for i in range(2))
            m = jnp.maximum(m0, m1)
            total = l0 * jnp.exp2((m0 - m) * EXPO) + l1 * jnp.exp2((m1 - m) * EXPO)
            cs[a, at_ : at_ + 1, :] = m
            cs[a, at_ + 1 : at_ + 2, :] = 1.0 / total

    def prob_of(s, m, inv):
        return jnp.exp2((s - m) * EXPO) * inv

    d3_s[...] = dot(lohi(z, y, 1)[0], gt[0, 0:HEAD, :])
    p3 = prob_of(s3_s[...], cs[0, 0:1, :], cs[0, 1:2, :])
    s3_s[...] = p3
    dk3[1] = dot(p3.astype(BF16), gn[0, :, 0:HEAD])
    for a in range(2):
        dl[a, 0:1, :] = zero if a else column_sum(p3 * d3_s[...])
        dl[a, 1:8, :] = jnp.zeros((7, rows), F32)

    def collect(gi, w, tiles, wide):
        zg = z_of(gi)
        dlo, dhi = [None] * NY, [None] * NY
        for a in range(2):
            x1, x2 = tiles(a)
            pick = picks(zg, a)
            one = dot(x1, wide[a, :, HEAD : 2 * HEAD])
            two = dot(x2, wide[a])
            for yy in range(NY):
                left, right = two[block(yy), 0:HEAD], two[block(yy), HEAD : 2 * HEAD]
                none_ = jnp.zeros_like(left)
                new_lo = one[block(yy), :] + jnp.where(pick[yy], left, none_)
                new_hi = jnp.where(pick[yy], none_, right)
                if a == 0:
                    here = jnp.logical_and(zg == z, yy == y)
                    dlo[yy], dhi[yy] = new_lo + jnp.where(here, dk3[w], none_), new_hi
                else:
                    dlo[yy], dhi[yy] = dlo[yy] + new_lo, dhi[yy] + new_hi
        for yy in range(NY):
            flip, _ = spans(ctx_of(zg, yy, core))
            out[zg, yy, w, 0:SPAN, :] = jnp.where(flip, dhi[yy], dlo[yy]).astype(BF16)
            out[zg, yy, w, SPAN : 2 * SPAN, :] = jnp.where(flip, dlo[yy], dhi[yy]).astype(BF16)

    def value_grads(gi):
        zg = z_of(gi)

        def tiles(a):
            pick = picks(zg, a)
            m_lo, i_lo, m_hi, i_hi = (cs[a, i : i + 1, :] for i in range(4))
            p1 = prob_of(s_s[gi, a, 0], m_hi, i_hi)
            s_s[gi, a, 0] = p1
            w2 = []
            for yy in range(NY):
                p2 = prob_of(
                    s_s[gi, a, 1, block(yy), :],
                    jnp.where(pick[yy], m_lo, m_hi),
                    jnp.where(pick[yy], i_lo, i_hi),
                )
                s_s[gi, a, 1, block(yy), :] = p2
                w2.append(p2.astype(BF16))
            return p1.astype(BF16), jnp.concatenate(w2, axis=0)

        collect(gi, 1, tiles, gn)

    def deltas(gi):
        zg = z_of(gi)
        for a in range(2):
            pick = picks(zg, a)
            e_lo = dl[a, 0:1, :]
            e_hi = dl[a, 1:2, :] + column_sum(s_s[gi, a, 0] * d_s[gi, a, 0])
            for yy in range(NY):
                part = column_sum(s_s[gi, a, 1, block(yy), :] * d_s[gi, a, 1, block(yy), :])
                e_lo = e_lo + jnp.where(pick[yy], part, zero)
                e_hi = e_hi + jnp.where(pick[yy], zero, part)
            dl[a, 0:1, :] = e_lo
            dl[a, 1:2, :] = e_hi

    def score_grad(p, d, delta):
        return (p * (d - delta) * SCALE).astype(BF16)

    def key_grads(gi):
        zg = z_of(gi)

        def tiles(a):
            pick = picks(zg, a)
            e_lo, e_hi = (dl[a, i : i + 1, :] + dl_in[1 - a, i : i + 1, :] for i in range(2))
            ds_s[gi, a, 0] = score_grad(s_s[gi, a, 0], d_s[gi, a, 0], e_hi)
            for yy in range(NY):
                ds_s[gi, a, 1, block(yy), :] = score_grad(
                    s_s[gi, a, 1, block(yy), :],
                    d_s[gi, a, 1, block(yy), :],
                    jnp.where(pick[yy], e_lo, e_hi),
                )
            return ds_s[gi, a, 0], ds_s[gi, a, 1]

        collect(gi, 0, tiles, qn)

    def query_step(gi, carry):
        for a in range(2):
            dqt[a] += dot(kc_s[gi, a].T, ds_s[gi, a, 1])
            dqt[a, HEAD : 2 * HEAD, :] += dot(klo_s[gi].T, ds_s[gi, a, 0])
        return carry

    def plus(a, b):
        return (a.astype(F32) + b.astype(F32)).astype(BF16)

    def ry_first(w, gi):
        zg = z_of(gi)
        if (w, gi) in RS_RELAY:
            remote(
                out.at[zg, y_op, w, low], ro.at[gi, w, low], yo_s.at[w, gi, 0], yo_r.at[w, gi, 0], dev_yu
            ).start()
            remote(
                out.at[zg, y_op, w, high], ro.at[gi, w, high], yo_s.at[w, gi, 1], yo_r.at[w, gi, 1], dev_yd
            ).start()
        else:
            ry_near(w, gi, 0)
            ry_near(w, gi, 1)
            remote(
                out.at[zg, y_op, w], ro.at[gi, w], yo_s.at[w, gi, 0], yo_r.at[w, gi, 0], dev_yo
            ).start()

    def ry_near(w, gi, i):
        b = out.at[z_of(gi), (y_up, y_dn)[i], w]
        remote(
            b, ry.at[gi, i, w], yf_s.at[w, gi, i], yf_r.at[w, gi, i], (dev_yu, dev_yd)[i]
        ).start()

    def ry_forward(w, gi):
        zg = z_of(gi)
        landed(ro.at[gi, w, low], yo_r.at[w, gi, 0])
        out[zg, y_up, w, low] = plus(out[zg, y_up, w, low], ro[gi, w, low])
        ry_near(w, gi, 0)
        landed(ro.at[gi, w, high], yo_r.at[w, gi, 1])
        out[zg, y_dn, w, high] = plus(out[zg, y_dn, w, high], ro[gi, w, high])
        ry_near(w, gi, 1)

    def ry_total(w, gi):
        zg = z_of(gi)
        landed(ry.at[gi, 0, w], yf_r.at[w, gi, 0])
        landed(ry.at[gi, 1, w], yf_r.at[w, gi, 1])
        total = out[zg, y, w].astype(F32) + ry[gi, 0, w].astype(F32) + ry[gi, 1, w].astype(F32)
        if (w, gi) not in RS_RELAY:
            landed(ro.at[gi, w], yo_r.at[w, gi, 0])
            total = total + ro[gi, w].astype(F32)
        zs[gi, w] = total.astype(BF16)
        for o in range(1 if gi == 0 else 0, tps):
            to = lax.rem(t + o, tps)
            to_rows = pl.ds(pl.multiple_of(to * tt, tt), tt)
            device = (ctx_of(zg, y, core), to)
            remote(
                zs.at[gi, w, to_rows], kvr.at[z, w, t], zr_s.at[w, gi], zr_r.at[w, z], device
            ).start()

    steps["forward"], steps["total"] = ry_forward, ry_total

    def z_first(gi):
        zg = z_of(gi)
        remote(
            out.at[zg, :, 1], rzv.at[gi - 1], zv_s.at[gi - 1], zv_r.at[gi - 1], (ctx_of(zg, y, core), t)
        ).start()

    def z_merge(w, gi):
        for i in range(2):
            landed(rzv.at[i], zv_r.at[i])
        for yy in range(NY):
            total = out[z, yy, w].astype(F32) + rzv[0, yy].astype(F32) + rzv[1, yy].astype(F32)
            out[z, yy, w] = total.astype(BF16)
        ry_first(w, gi)

    steps["merge"] = z_merge

    def value_step(i, carry):
        gi = lax.rem(i + 1, NZ)
        value_grads(gi)
        for g in range(1 if Z_FIRST else 0, NZ):
            pl.when(gi == g)(
                functools.partial(z_first, g) if g in Z_FIRST else functools.partial(ry_first, 1, g)
            )
        return carry

    lax.fori_loop(0, NZ, value_step, 0)

    def delta_step(gi, carry):
        for g in range(INNER_AHEAD, NZ):
            pl.when(gi == g)(functools.partial(y_done, 1, g))

        @pl.when(gi >= INNER_AHEAD)
        def _():
            inner(gi)

        deltas(gi)
        return carry

    lax.fori_loop(0, NZ, delta_step, 0)

    dl_copy = remote(dl, dl_in, pair_s.at[4], pair_r.at[4], dev_pair)
    dl_copy.start()
    act("delta")
    dl_copy.wait_recv()
    ds3 = score_grad(s3_s[...], d3_s[...], dl[0, 0:1, :] + dl_in[1, 0:1, :])
    dk3[0] = dot(ds3, qn[0, :, 0:HEAD])
    dqt[0, 0:HEAD, :] = dot(lohi(z, y, 0)[0].T, ds3)

    def key_step(i, carry):
        gi = NZ - 1 - i
        key_grads(gi)
        at(gi, functools.partial(ry_first, 0))
        point("key", i)
        return carry

    lax.fori_loop(0, NZ, key_step, 0)

    act("keys")
    lax.fori_loop(0, NZ, query_step, 0)
    dqsend[...] = dqt[1].astype(BF16)
    dq_copy = remote(dqsend, dqrecv, pair_s.at[3], pair_r.at[3], dev_pair)
    dq_copy.start()
    act("last")
    dq_copy.wait_recv()
    total_q = dqt[0] + dqrecv[...].astype(F32)
    lo, hi = total_q[0:HEAD, :].T.astype(BF16), total_q[HEAD : 2 * HEAD, :].T.astype(BF16)
    first, second = jnp.where(flips[0], hi, lo), jnp.where(flips[0], lo, hi)
    for h in range(heads):
        dq_out[0:SPAN, h * HEAD : (h + 1) * HEAD] = first[h * SPAN : (h + 1) * SPAN, :]
        dq_out[SPAN : 2 * SPAN, h * HEAD : (h + 1) * HEAD] = second[h * SPAN : (h + 1) * SPAN, :]
    act("end")
    for w in range(2):
        kvr[z, w, t] = zs[0, w, own_rows]

    for copy in (q_copy, g_copy, st_copy, dl_copy, dq_copy):
        copy.wait_send()
    whole = kv.at[0, 0, 0]
    half = kv.at[0, 0, 0, low]
    pieces = [kvst.at[0, pl.ds(0, tps - 1)]] + [kvst.at[0]] * (NZ - 1)
    for w in range(2):
        for gi in range(NZ):
            landed(pieces[gi], zt_s.at[w, gi])
            straight = w == 0 or gi not in Z_FIRST
            if straight:
                landed(pieces[gi], zr_s.at[w, gi])
            relay = (w, gi) in AG_RELAY
            for i in range(4 if relay else 3):
                landed(half if relay and i >= 2 else whole, ysem_s.at[w, gi, i])
            relay = (w, gi) in RS_RELAY
            for i in range(2 if relay else 1):
                if straight:
                    landed(half if relay else whole, yo_s.at[w, gi, i])
            for i in range(2):
                if straight:
                    landed(whole, yf_s.at[w, gi, i])
    for i in range(len(Z_FIRST)):
        landed(rzv.at[i], zv_s.at[i])
    for w, result in ((1, v_out), (0, k_out)):
        parts = [gi for gi in (3, 2, 1, 0) if w == 0 or gi not in Z_FIRST]
        for gi in parts:
            landed(pieces[gi], zr_r.at[w, z_of(gi)])
        for g in range(tps):
            total = sum(kvr[z_of(gi), w, g].astype(F32) for gi in parts)
            result[:, g * HEAD : (g + 1) * HEAD] = total.astype(BF16)


def body(queries, keys, values, output_gradient, span_order):
    tps = lax.axis_size("tp")
    toks, width = queries.shape
    heads = width // HEAD
    rows = heads * SPAN
    tt = keys.shape[0]
    vmem = pltpu.VMEM
    half = (toks, HEAD)
    block = (2, *half)
    group = NY * SPAN
    dma = pltpu.SemaphoreType.DMA
    scratch = [
        vmem((2, tps, tt, HEAD), BF16),
        vmem((NZ, NY, *block), BF16),
        vmem((2, heads, *half), BF16),
        vmem((2, heads, *half), BF16),
        vmem((2, rows, 2 * HEAD), BF16),
        vmem((2, rows, 2 * HEAD), BF16),
        vmem((2, 2 * HEAD, rows), BF16),
        vmem((2, 2 * HEAD, rows), BF16),
        vmem((NZ, group, HEAD), BF16),
        vmem((NZ, 2, group, 2 * HEAD), BF16),
        vmem((NZ, group, HEAD), BF16),
        vmem((NZ, 2, group, 2 * HEAD), BF16),
        vmem((NZ, 2, 2, group, rows), F32),
        vmem((NZ, 2, 2, group, rows), F32),
        vmem((NZ, 2, 2, group, rows), BF16),
        vmem((SPAN, rows), F32),
        vmem((SPAN, rows), F32),
        vmem((2, 8, rows), F32),
        vmem((2, 8, rows), F32),
        vmem((2, 8, rows), F32),
        vmem((2, 8, rows), F32),
        vmem((2, 8, rows), F32),
        vmem((2, 2 * HEAD, rows), F32),
        vmem((2, SPAN, HEAD), F32),
        vmem((2 * HEAD, rows), BF16),
        vmem((2 * HEAD, rows), BF16),
        vmem((NZ, NY, *block), BF16),
        vmem((NZ, *block), BF16),
        vmem((NZ, 2, *block), BF16),
        vmem((NZ, *block), BF16),
        vmem((NZ, 2, tps, tt, HEAD), BF16),
        vmem((2, NY, *half), BF16),
        dma((4,)),
        dma((2, NZ)),
        dma((2, NZ)),
        dma((2, NZ, 4)),
        dma((2, NZ, 4)),
        dma((5,)),
        dma((5,)),
        dma((2, NZ, 2)),
        dma((2, NZ, 2)),
        dma((2, NZ, 2)),
        dma((2, NZ, 2)),
        dma((2, NZ)),
        dma((2, NZ)),
        dma((2,)),
        dma((2,)),
    ]
    anywhere = pl.BlockSpec(memory_space=pl.ANY)
    in_vmem = pl.BlockSpec(memory_space=pltpu.VMEM)
    shapes = (queries.shape, keys.shape, values.shape)
    grads = pl.pallas_call(
        functools.partial(kernel, tps, heads),
        out_shape=tuple(pltpu.VMEM(shape, BF16) for shape in shapes),
        in_specs=[pl.BlockSpec(memory_space=pltpu.SMEM)] + [anywhere] * 4,
        out_specs=(in_vmem,) * 3,
        scratch_shapes=scratch,
        compiler_params=pltpu.CompilerParams(
            collective_id=0, has_side_effects=True, vmem_limit_bytes=56 * 1024 * 1024
        ),
    )(span_order, queries, keys, values, output_gradient)
    return tuple(
        pl.pallas_call(
            put_out,
            out_shape=tuple(jax.ShapeDtypeStruct(shape, BF16) for shape in shapes),
            in_specs=[in_vmem] * 3,
            out_specs=(anywhere,) * 3,
            scratch_shapes=[dma((3,))],
            compiler_params=pltpu.CompilerParams(vmem_limit_bytes=2 * 1024 * 1024),
        )(*grads)
    )


def put_out(a, b, c, x, y, z, sems):
    copies = [
        pltpu.make_async_copy(src, dst, sems.at[i])
        for i, (src, dst) in enumerate(((a, x), (b, y), (c, z)))
    ]
    for copy in copies:
        copy.start()
    for copy in copies:
        copy.wait()


def solution(mesh):
    return jax.shard_map(
        body,
        mesh=mesh,
        in_specs=(
            P("ctx", "tp"),
            P(("ctx", "tp"), None),
            P(("ctx", "tp"), None),
            P("ctx", "tp"),
            P(),
        ),
        out_specs=(P("ctx", "tp"), P(("ctx", "tp"), None), P(("ctx", "tp"), None)),
        check_vma=False,
    )
```

```python
import functools
import math

import jax
import jax.numpy as jnp
from jax import lax
from jax.experimental import pallas as pl
from jax.experimental.pallas import tpu as pltpu
from jax.sharding import PartitionSpec as P

HEAD = 128
SPAN = 64
KV_HEADS = 8
NY = 4
NZ = 4
SCALE = HEAD**-0.5
EXPO = SCALE * math.log2(math.e)
NEG = -1e30
ZT_FIRST = ((0, 0), (0, 1), (0, 2), (0, 3))
AG_RELAY = ()
INNER_AHEAD = 1
Z_FIRST = ()
RS_RELAY = ()
POINTS = {'early': (('zt', 1, 0), ('zt', 1, 1, 0), ('zt', 1, 2, 0), ('zt', 1, 3, 0)), 'first': (('pair', 0, 0), ('send', 1, 0, 0)), 'second': (('pair', 1, 0),), 'third': (('zt', 1, 1, 1), ('zt', 1, 2, 1), ('zt', 1, 3, 1)), 'score': {0: (('send', 1, 1, 0), ('send', 1, 0, 1)), 1: (('send', 1, 2, 0),), 2: (('send', 1, 3, 0), ('send', 1, 1, 1)), 3: (('send', 1, 2, 1), ('send', 1, 3, 1))}, 'stats': (('inner', 1, 0),), 'value': {}, 'delta': (), 'key': {0: (('total', 1, 3),), 1: (('total', 1, 2),), 2: (('total', 1, 1),), 3: (('total', 1, 0),)}, 'keys': (), 'last': (('total', 0, 3), ('total', 0, 2)), 'end': (('total', 0, 1), ('total', 0, 0))}
MESH = pl.DeviceIdType.MESH
F32 = jnp.float32
BF16 = jnp.bfloat16


def dot(a, b):
    return jnp.dot(a, b, preferred_element_type=F32)


def kernel(
    tps,
    heads,
    span,
    q_hbm,
    k_hbm,
    v_hbm,
    g_hbm,
    dq_out,
    k_out,
    v_out,
    kvst,
    kv,
    qs,
    gs,
    qn,
    gn,
    qt,
    gt,
    klo_s,
    kc_s,
    vlo_s,
    vc_s,
    s_s,
    d_s,
    ds_s,
    s3_s,
    d3_s,
    st,
    st_in,
    cs,
    dl,
    dl_in,
    dqt,
    dk3,
    dqsend,
    dqrecv,
    out,
    ro,
    ry,
    zs,
    kvr,
    rzv,
    loc,
    zt_s,
    zt_r,
    ysem_s,
    ysem_r,
    pair_s,
    pair_r,
    yo_s,
    yo_r,
    yf_s,
    yf_r,
    zr_s,
    zr_r,
    zv_s,
    zv_r,
):
    rows = heads * SPAN
    toks = 2 * SPAN
    tt = toks // tps
    c = lax.axis_index("ctx")
    t = lax.axis_index("tp")
    core = lax.rem(c, 2)
    y = lax.rem(c // 2, NY)
    z = c // (2 * NY)

    def ctx_of(zz, yy, cc):
        return (zz * NY + yy) * 2 + cc

    y_up, y_dn, y_op = lax.rem(y + 1, NY), lax.rem(y + 3, NY), lax.rem(y + 2, NY)
    dev_yu, dev_yd = (ctx_of(z, y_up, core), t), (ctx_of(z, y_dn, core), t)
    dev_yo = (ctx_of(z, y_op, core), t)
    dev_pair = (ctx_of(z, y, 1 - core), t)

    def remote(src, dst, send, recv, device):
        return pltpu.make_async_remote_copy(
            src_ref=src,
            dst_ref=dst,
            send_sem=send,
            recv_sem=recv,
            device_id=device,
            device_id_type=MESH,
        )

    def landed(ref, sem):
        pltpu.make_async_copy(ref, ref, sem).wait()

    own_rows = pl.ds(pl.multiple_of(t * tt, tt), tt)
    own_cols = pl.ds(pl.multiple_of(t * HEAD, HEAD), HEAD)

    def fetch(w, hbm):
        for g in range(tps):
            pltpu.make_async_copy(
                hbm.at[:, pl.ds(g * HEAD, HEAD)], kvst.at[w, g], loc.at[w]
            ).start()
        pltpu.make_async_copy(
            hbm.at[:, own_cols], kv.at[z, y, w, own_rows], zt_r.at[w, z]
        ).start()

    fetch(0, k_hbm)

    def z_of(gi):
        return lax.rem(z + gi + (gi // 2) * (1 - 2 * (gi % 2)), NZ)

    def greet(device):
        pl.semaphore_signal(barrier, inc=1, device_id=device, device_id_type=MESH)

    barrier = pltpu.get_barrier_semaphore()
    for gi in range(NZ):
        for o in range(1 if gi == 0 else 0, tps):
            greet((ctx_of(z_of(gi), y, core), lax.rem(t + o, tps)))
    for device in (dev_yu, dev_yd, dev_yo, dev_pair):
        greet(device)
    fetch(1, v_hbm)
    landed(kvst.at[0], loc.at[0])
    pl.semaphore_wait(barrier, NZ * tps - 1 + 4)

    def zt_send(w, gi):
        if (w, gi) == (1, 0):
            landed(kvst.at[1], loc.at[1])
        for o in range(1 if gi == 0 else 0, tps):
            to = lax.rem(t + o, tps)
            device = (ctx_of(z_of(gi), y, core), to)
            remote(
                kvst.at[w, to], kv.at[z, y, w, own_rows], zt_s.at[w, gi], zt_r.at[w, z], device
            ).start()

    for w, gi in ZT_FIRST:
        zt_send(w, gi)
    for h in range(heads):
        cols = pl.ds(h * HEAD, HEAD)
        pltpu.make_async_copy(q_hbm.at[:, cols], qs.at[0, h], loc.at[2]).start()
        pltpu.make_async_copy(g_hbm.at[:, cols], gs.at[0, h], loc.at[3]).start()
    pairs = [(qs, remote(qs.at[0], qs.at[1], pair_s.at[0], pair_r.at[0], dev_pair))]
    pairs.append((gs, remote(gs.at[0], gs.at[1], pair_s.at[1], pair_r.at[1], dev_pair)))
    q_copy, g_copy = pairs[0][1], pairs[1][1]

    def pair_send(w, gi):
        landed(pairs[w][0].at[0], loc.at[2 + w])
        pairs[w][1].start()

    def spans(cc):
        s0, s1 = span[2 * cc], span[2 * cc + 1]
        return s0 > s1, jnp.minimum(s0, s1)

    devs = (c, ctx_of(z, y, 1 - core))
    flips, lows = zip(*[spans(d) for d in devs])

    def prepare(a, src, normal, turned):
        first = src[a, :, 0:SPAN, :].reshape(rows, HEAD)
        second = src[a, :, SPAN : 2 * SPAN, :].reshape(rows, HEAD)
        lo = jnp.where(flips[a], second, first)
        hi = jnp.where(flips[a], first, second)
        normal[a, :, 0:HEAD] = lo
        normal[a, :, HEAD : 2 * HEAD] = hi
        turned[a, 0:HEAD, :] = lo.T
        turned[a, HEAD : 2 * HEAD, :] = hi.T

    low, high = pl.ds(0, SPAN), pl.ds(SPAN, SPAN)

    def y_send(w, gi):
        zg = z_of(gi)
        b = kv.at[zg, y, w]
        landed(b, zt_r.at[w, zg])
        remote(b, b, ysem_s.at[w, gi, 0], ysem_r.at[w, gi, 0], dev_yu).start()
        remote(b, b, ysem_s.at[w, gi, 1], ysem_r.at[w, gi, 1], dev_yd).start()
        if (w, gi) not in AG_RELAY:
            remote(b, b, ysem_s.at[w, gi, 2], ysem_r.at[w, gi, 2], dev_yo).start()

    def y_relay(w, gi):
        zg = z_of(gi)
        landed(kv.at[zg, y_dn, w], ysem_r.at[w, gi, 0])
        b = kv.at[zg, y_dn, w, low]
        remote(b, b, ysem_s.at[w, gi, 2], ysem_r.at[w, gi, 2], dev_yu).start()
        landed(kv.at[zg, y_up, w], ysem_r.at[w, gi, 1])
        b = kv.at[zg, y_up, w, high]
        remote(b, b, ysem_s.at[w, gi, 3], ysem_r.at[w, gi, 3], dev_yd).start()

    def y_done(w, gi):
        zg = z_of(gi)
        if (w, gi) in AG_RELAY:
            landed(kv.at[zg, y_op, w, low], ysem_r.at[w, gi, 2])
            landed(kv.at[zg, y_op, w, high], ysem_r.at[w, gi, 3])
        else:
            landed(kv.at[zg, y_dn, w], ysem_r.at[w, gi, 0])
            landed(kv.at[zg, y_up, w], ysem_r.at[w, gi, 1])
            landed(kv.at[zg, y_op, w], ysem_r.at[w, gi, 2])

    steps = {}

    def act(name, g=None):
        for step, w, gi, *only in POINTS[name] if g is None else POINTS[name].get(g, ()):
            todo = functools.partial(steps[step], w, gi)
            if only:
                pl.when(core == only[0])(todo)
            else:
                todo()

    def point(name, i):
        for g in POINTS[name]:
            pl.when(i == g)(functools.partial(act, name, g))

    def at(gi, todo):
        for g in range(NZ):
            pl.when(gi == g)(functools.partial(todo, g))

    steps["relay"], steps["send"] = y_relay, y_send
    steps["zt"], steps["pair"] = zt_send, pair_send
    act("early")
    y_send(0, 0)
    act("first")
    prepare(0, qs, qn, qt)
    y_send(0, 1)
    y_send(0, 2)
    act("second")

    def lohi(zg, yy, w):
        first, second = kv[zg, yy, w, 0:SPAN, :], kv[zg, yy, w, SPAN : 2 * SPAN, :]
        flip, _ = spans(ctx_of(zg, yy, core))
        return jnp.where(flip, second, first), jnp.where(flip, first, second)

    key_i = lax.broadcasted_iota(jnp.int32, (SPAN, rows), 0)
    tok_i = lax.rem(lax.broadcasted_iota(jnp.int32, (SPAN, rows), 1), SPAN)
    hidden = key_i > tok_i

    s3 = jnp.where(hidden, NEG, dot(lohi(z, y, 0)[0], qt[0, 0:HEAD, :]))
    s3_s[...] = s3
    m3 = jnp.max(s3, axis=0, keepdims=True)
    e3 = jnp.exp2((s3 - m3) * EXPO)
    none = jnp.full((1, rows), NEG, F32)
    zero = jnp.zeros((1, rows), F32)
    for a in range(2):
        st[a, 0:1, :] = none if a else m3
        st[a, 1:2, :] = zero if a else jnp.sum(e3, axis=0, keepdims=True)
        st[a, 2:3, :] = none
        st[a, 3:8, :] = jnp.zeros((5, rows), F32)
    y_send(0, 3)
    act("third")
    prepare(0, gs, gn, gt)
    q_copy.wait_recv()
    prepare(1, qs, qn, qt)
    def picks(zg, a):
        return [spans(ctx_of(zg, yy, core))[1] < lows[a] for yy in range(NY)]

    def block(yy):
        return slice(yy * SPAN, (yy + 1) * SPAN)

    def split(zg, w, lo_s, cat_s, gi):
        pairs = [lohi(zg, yy, w) for yy in range(NY)]
        for yy in range(NY):
            lo_s[gi, block(yy), :] = pairs[yy][0]
        for a in range(2):
            pick = picks(zg, a)
            for yy in range(NY):
                lo, hi = pairs[yy]
                none_ = jnp.zeros_like(lo)
                cat_s[gi, a, block(yy), 0:HEAD] = jnp.where(pick[yy], lo, none_)
                cat_s[gi, a, block(yy), HEAD : 2 * HEAD] = jnp.where(pick[yy], none_, hi)

    def column_sum(x):
        return jnp.sum(x, axis=0, keepdims=True)

    def scores(gi):
        zg = z_of(gi)
        split(zg, 0, klo_s, kc_s, gi)
        for a in range(2):
            pick = picks(zg, a)
            s1 = dot(klo_s[gi], qt[a, HEAD : 2 * HEAD, :])
            s2 = dot(kc_s[gi, a], qt[a])
            s_s[gi, a, 0] = s1
            parts = []
            for yy in range(NY):
                part = s2[block(yy), :]
                if a == 0:
                    here = jnp.logical_and(zg == z, yy == y)
                    part = jnp.where(jnp.logical_and(hidden, here), NEG, part)
                s_s[gi, a, 1, block(yy), :] = part
                parts.append(part)
            m_lo, l_lo, m_hi, l_hi = (st[a, i : i + 1, :] for i in range(4))
            n_lo, n_hi = m_lo, jnp.maximum(m_hi, jnp.max(s1, axis=0, keepdims=True))
            for yy in range(NY):
                top = jnp.max(parts[yy], axis=0, keepdims=True)
                n_lo = jnp.maximum(n_lo, jnp.where(pick[yy], top, none))
                n_hi = jnp.maximum(n_hi, jnp.where(pick[yy], none, top))
            l_lo = l_lo * jnp.exp2((m_lo - n_lo) * EXPO)
            l_hi = l_hi * jnp.exp2((m_hi - n_hi) * EXPO)
            l_hi = l_hi + column_sum(jnp.exp2((s1 - n_hi) * EXPO))
            for yy in range(NY):
                e2 = jnp.exp2((parts[yy] - jnp.where(pick[yy], n_lo, n_hi)) * EXPO)
                total = column_sum(e2)
                l_lo = l_lo + jnp.where(pick[yy], total, zero)
                l_hi = l_hi + jnp.where(pick[yy], zero, total)
            for i, x in enumerate((n_lo, l_lo, n_hi, l_hi)):
                st[a, i : i + 1, :] = x

    def inner(gi):
        split(z_of(gi), 1, vlo_s, vc_s, gi)
        for a in range(2):
            d_s[gi, a, 0] = dot(vlo_s[gi], gt[a, HEAD : 2 * HEAD, :])
            d_s[gi, a, 1] = dot(vc_s[gi, a], gt[a])

    def inner_now(w, gi):
        y_done(w, gi)
        inner(gi)

    steps["inner"] = inner_now

    def score_step(gi, carry):
        at(gi, functools.partial(y_done, 0))
        scores(gi)
        point("score", gi)
        return carry

    lax.fori_loop(0, NZ, score_step, 0)

    st_copy = remote(st, st_in, pair_s.at[2], pair_r.at[2], dev_pair)
    st_copy.start()
    dqt[...] = jnp.zeros_like(dqt)
    g_copy.wait_recv()
    prepare(1, gs, gn, gt)
    act("stats")
    st_copy.wait_recv()
    for a in range(2):
        for at_ in (0, 2):
            m0, l0 = (st[a, at_ + i : at_ + i + 1, :] for i in range(2))
            m1, l1 = (st_in[1 - a, at_ + i : at_ + i + 1, :] for i in range(2))
            m = jnp.maximum(m0, m1)
            total = l0 * jnp.exp2((m0 - m) * EXPO) + l1 * jnp.exp2((m1 - m) * EXPO)
            cs[a, at_ : at_ + 1, :] = m
            cs[a, at_ + 1 : at_ + 2, :] = 1.0 / total

    def prob_of(s, m, inv):
        return jnp.exp2((s - m) * EXPO) * inv

    d3_s[...] = dot(lohi(z, y, 1)[0], gt[0, 0:HEAD, :])
    p3 = prob_of(s3_s[...], cs[0, 0:1, :], cs[0, 1:2, :])
    s3_s[...] = p3
    dk3[1] = dot(p3.astype(BF16), gn[0, :, 0:HEAD])
    for a in range(2):
        dl[a, 0:1, :] = zero if a else column_sum(p3 * d3_s[...])
        dl[a, 1:8, :] = jnp.zeros((7, rows), F32)

    def collect(gi, w, tiles, wide):
        zg = z_of(gi)
        dlo, dhi = [None] * NY, [None] * NY
        for a in range(2):
            x1, x2 = tiles(a)
            pick = picks(zg, a)
            one = dot(x1, wide[a, :, HEAD : 2 * HEAD])
            two = dot(x2, wide[a])
            for yy in range(NY):
                left, right = two[block(yy), 0:HEAD], two[block(yy), HEAD : 2 * HEAD]
                none_ = jnp.zeros_like(left)
                new_lo = one[block(yy), :] + jnp.where(pick[yy], left, none_)
                new_hi = jnp.where(pick[yy], none_, right)
                if a == 0:
                    here = jnp.logical_and(zg == z, yy == y)
                    dlo[yy], dhi[yy] = new_lo + jnp.where(here, dk3[w], none_), new_hi
                else:
                    dlo[yy], dhi[yy] = dlo[yy] + new_lo, dhi[yy] + new_hi
        for yy in range(NY):
            flip, _ = spans(ctx_of(zg, yy, core))
            out[zg, yy, w, 0:SPAN, :] = jnp.where(flip, dhi[yy], dlo[yy]).astype(BF16)
            out[zg, yy, w, SPAN : 2 * SPAN, :] = jnp.where(flip, dlo[yy], dhi[yy]).astype(BF16)

    def value_grads(gi):
        zg = z_of(gi)

        def tiles(a):
            pick = picks(zg, a)
            m_lo, i_lo, m_hi, i_hi = (cs[a, i : i + 1, :] for i in range(4))
            p1 = prob_of(s_s[gi, a, 0], m_hi, i_hi)
            s_s[gi, a, 0] = p1
            w2 = []
            for yy in range(NY):
                p2 = prob_of(
                    s_s[gi, a, 1, block(yy), :],
                    jnp.where(pick[yy], m_lo, m_hi),
                    jnp.where(pick[yy], i_lo, i_hi),
                )
                s_s[gi, a, 1, block(yy), :] = p2
                w2.append(p2.astype(BF16))
            return p1.astype(BF16), jnp.concatenate(w2, axis=0)

        collect(gi, 1, tiles, gn)

    def deltas(gi):
        zg = z_of(gi)
        for a in range(2):
            pick = picks(zg, a)
            e_lo = dl[a, 0:1, :]
            e_hi = dl[a, 1:2, :] + column_sum(s_s[gi, a, 0] * d_s[gi, a, 0])
            for yy in range(NY):
                part = column_sum(s_s[gi, a, 1, block(yy), :] * d_s[gi, a, 1, block(yy), :])
                e_lo = e_lo + jnp.where(pick[yy], part, zero)
                e_hi = e_hi + jnp.where(pick[yy], zero, part)
            dl[a, 0:1, :] = e_lo
            dl[a, 1:2, :] = e_hi

    def score_grad(p, d, delta):
        return (p * (d - delta) * SCALE).astype(BF16)

    def key_grads(gi):
        zg = z_of(gi)

        def tiles(a):
            pick = picks(zg, a)
            e_lo, e_hi = (dl[a, i : i + 1, :] + dl_in[1 - a, i : i + 1, :] for i in range(2))
            ds_s[gi, a, 0] = score_grad(s_s[gi, a, 0], d_s[gi, a, 0], e_hi)
            for yy in range(NY):
                ds_s[gi, a, 1, block(yy), :] = score_grad(
                    s_s[gi, a, 1, block(yy), :],
                    d_s[gi, a, 1, block(yy), :],
                    jnp.where(pick[yy], e_lo, e_hi),
                )
            return ds_s[gi, a, 0], ds_s[gi, a, 1]

        collect(gi, 0, tiles, qn)

    def query_step(gi, carry):
        for a in range(2):
            dqt[a] += dot(kc_s[gi, a].T, ds_s[gi, a, 1])
            dqt[a, HEAD : 2 * HEAD, :] += dot(klo_s[gi].T, ds_s[gi, a, 0])
        return carry

    def plus(a, b):
        return (a.astype(F32) + b.astype(F32)).astype(BF16)

    def ry_first(w, gi):
        zg = z_of(gi)
        if (w, gi) in RS_RELAY:
            remote(
                out.at[zg, y_op, w, low], ro.at[gi, w, low], yo_s.at[w, gi, 0], yo_r.at[w, gi, 0], dev_yu
            ).start()
            remote(
                out.at[zg, y_op, w, high], ro.at[gi, w, high], yo_s.at[w, gi, 1], yo_r.at[w, gi, 1], dev_yd
            ).start()
        else:
            ry_near(w, gi, 0)
            ry_near(w, gi, 1)
            remote(
                out.at[zg, y_op, w], ro.at[gi, w], yo_s.at[w, gi, 0], yo_r.at[w, gi, 0], dev_yo
            ).start()

    def ry_near(w, gi, i):
        b = out.at[z_of(gi), (y_up, y_dn)[i], w]
        remote(
            b, ry.at[gi, i, w], yf_s.at[w, gi, i], yf_r.at[w, gi, i], (dev_yu, dev_yd)[i]
        ).start()

    def ry_forward(w, gi):
        zg = z_of(gi)
        landed(ro.at[gi, w, low], yo_r.at[w, gi, 0])
        out[zg, y_up, w, low] = plus(out[zg, y_up, w, low], ro[gi, w, low])
        ry_near(w, gi, 0)
        landed(ro.at[gi, w, high], yo_r.at[w, gi, 1])
        out[zg, y_dn, w, high] = plus(out[zg, y_dn, w, high], ro[gi, w, high])
        ry_near(w, gi, 1)

    def ry_total(w, gi):
        zg = z_of(gi)
        landed(ry.at[gi, 0, w], yf_r.at[w, gi, 0])
        landed(ry.at[gi, 1, w], yf_r.at[w, gi, 1])
        total = out[zg, y, w].astype(F32) + ry[gi, 0, w].astype(F32) + ry[gi, 1, w].astype(F32)
        if (w, gi) not in RS_RELAY:
            landed(ro.at[gi, w], yo_r.at[w, gi, 0])
            total = total + ro[gi, w].astype(F32)
        zs[gi, w] = total.astype(BF16)
        for o in range(1 if gi == 0 else 0, tps):
            to = lax.rem(t + o, tps)
            to_rows = pl.ds(pl.multiple_of(to * tt, tt), tt)
            device = (ctx_of(zg, y, core), to)
            remote(
                zs.at[gi, w, to_rows], kvr.at[z, w, t], zr_s.at[w, gi], zr_r.at[w, z], device
            ).start()

    steps["forward"], steps["total"] = ry_forward, ry_total

    def z_first(gi):
        zg = z_of(gi)
        remote(
            out.at[zg, :, 1], rzv.at[gi - 1], zv_s.at[gi - 1], zv_r.at[gi - 1], (ctx_of(zg, y, core), t)
        ).start()

    def z_merge(w, gi):
        for i in range(2):
            landed(rzv.at[i], zv_r.at[i])
        for yy in range(NY):
            total = out[z, yy, w].astype(F32) + rzv[0, yy].astype(F32) + rzv[1, yy].astype(F32)
            out[z, yy, w] = total.astype(BF16)
        ry_first(w, gi)

    steps["merge"], steps["open"] = z_merge, ry_first

    def value_step(i, carry):
        gi = NZ - 1 - i
        value_grads(gi)
        for g in range(1 if Z_FIRST else 0, NZ):
            pl.when(gi == g)(
                functools.partial(z_first, g) if g in Z_FIRST else functools.partial(ry_first, 1, g)
            )
        return carry

    lax.fori_loop(0, NZ, value_step, 0)

    def delta_step(gi, carry):
        for g in range(INNER_AHEAD, NZ):
            pl.when(gi == g)(functools.partial(y_done, 1, g))

        @pl.when(gi >= INNER_AHEAD)
        def _():
            inner(gi)

        deltas(gi)
        return carry

    lax.fori_loop(0, NZ, delta_step, 0)

    dl_copy = remote(dl, dl_in, pair_s.at[4], pair_r.at[4], dev_pair)
    dl_copy.start()
    act("delta")
    dl_copy.wait_recv()
    ds3 = score_grad(s3_s[...], d3_s[...], dl[0, 0:1, :] + dl_in[1, 0:1, :])
    dk3[0] = dot(ds3, qn[0, :, 0:HEAD])
    dqt[0, 0:HEAD, :] = dot(lohi(z, y, 0)[0].T, ds3)

    def key_step(i, carry):
        gi = NZ - 1 - i
        key_grads(gi)
        at(gi, functools.partial(ry_first, 0))
        point("key", i)
        return carry

    lax.fori_loop(0, NZ, key_step, 0)

    act("keys")
    lax.fori_loop(0, NZ, query_step, 0)
    dqsend[...] = dqt[1].astype(BF16)
    dq_copy = remote(dqsend, dqrecv, pair_s.at[3], pair_r.at[3], dev_pair)
    dq_copy.start()
    act("last")
    dq_copy.wait_recv()
    total_q = dqt[0] + dqrecv[...].astype(F32)
    lo, hi = total_q[0:HEAD, :].T.astype(BF16), total_q[HEAD : 2 * HEAD, :].T.astype(BF16)
    first, second = jnp.where(flips[0], hi, lo), jnp.where(flips[0], lo, hi)
    for h in range(heads):
        dq_out[0:SPAN, h * HEAD : (h + 1) * HEAD] = first[h * SPAN : (h + 1) * SPAN, :]
        dq_out[SPAN : 2 * SPAN, h * HEAD : (h + 1) * HEAD] = second[h * SPAN : (h + 1) * SPAN, :]
    act("end")
    for w in range(2):
        kvr[z, w, t] = zs[0, w, own_rows]

    for copy in (q_copy, g_copy, st_copy, dl_copy, dq_copy):
        copy.wait_send()
    whole = kv.at[0, 0, 0]
    half = kv.at[0, 0, 0, low]
    pieces = [kvst.at[0, pl.ds(0, tps - 1)]] + [kvst.at[0]] * (NZ - 1)
    for w in range(2):
        for gi in range(NZ):
            landed(pieces[gi], zt_s.at[w, gi])
            straight = w == 0 or gi not in Z_FIRST
            if straight:
                landed(pieces[gi], zr_s.at[w, gi])
            relay = (w, gi) in AG_RELAY
            for i in range(4 if relay else 3):
                landed(half if relay and i >= 2 else whole, ysem_s.at[w, gi, i])
            relay = (w, gi) in RS_RELAY
            for i in range(2 if relay else 1):
                if straight:
                    landed(half if relay else whole, yo_s.at[w, gi, i])
            for i in range(2):
                if straight:
                    landed(whole, yf_s.at[w, gi, i])
    for i in range(len(Z_FIRST)):
        landed(rzv.at[i], zv_s.at[i])
    for w, result in ((1, v_out), (0, k_out)):
        parts = [gi for gi in (3, 2, 1, 0) if w == 0 or gi not in Z_FIRST]
        for gi in parts:
            landed(pieces[gi], zr_r.at[w, z_of(gi)])
        for g in range(tps):
            total = sum(kvr[z_of(gi), w, g].astype(F32) for gi in parts)
            result[:, g * HEAD : (g + 1) * HEAD] = total.astype(BF16)


def body(queries, keys, values, output_gradient, span_order):
    tps = lax.axis_size("tp")
    toks, width = queries.shape
    heads = width // HEAD
    rows = heads * SPAN
    tt = keys.shape[0]
    vmem = pltpu.VMEM
    half = (toks, HEAD)
    block = (2, *half)
    group = NY * SPAN
    dma = pltpu.SemaphoreType.DMA
    scratch = [
        vmem((2, tps, tt, HEAD), BF16),
        vmem((NZ, NY, *block), BF16),
        vmem((2, heads, *half), BF16),
        vmem((2, heads, *half), BF16),
        vmem((2, rows, 2 * HEAD), BF16),
        vmem((2, rows, 2 * HEAD), BF16),
        vmem((2, 2 * HEAD, rows), BF16),
        vmem((2, 2 * HEAD, rows), BF16),
        vmem((NZ, group, HEAD), BF16),
        vmem((NZ, 2, group, 2 * HEAD), BF16),
        vmem((NZ, group, HEAD), BF16),
        vmem((NZ, 2, group, 2 * HEAD), BF16),
        vmem((NZ, 2, 2, group, rows), F32),
        vmem((NZ, 2, 2, group, rows), F32),
        vmem((NZ, 2, 2, group, rows), BF16),
        vmem((SPAN, rows), F32),
        vmem((SPAN, rows), F32),
        vmem((2, 8, rows), F32),
        vmem((2, 8, rows), F32),
        vmem((2, 8, rows), F32),
        vmem((2, 8, rows), F32),
        vmem((2, 8, rows), F32),
        vmem((2, 2 * HEAD, rows), F32),
        vmem((2, SPAN, HEAD), F32),
        vmem((2 * HEAD, rows), BF16),
        vmem((2 * HEAD, rows), BF16),
        vmem((NZ, NY, *block), BF16),
        vmem((NZ, *block), BF16),
        vmem((NZ, 2, *block), BF16),
        vmem((NZ, *block), BF16),
        vmem((NZ, 2, tps, tt, HEAD), BF16),
        vmem((2, NY, *half), BF16),
        dma((4,)),
        dma((2, NZ)),
        dma((2, NZ)),
        dma((2, NZ, 4)),
        dma((2, NZ, 4)),
        dma((5,)),
        dma((5,)),
        dma((2, NZ, 2)),
        dma((2, NZ, 2)),
        dma((2, NZ, 2)),
        dma((2, NZ, 2)),
        dma((2, NZ)),
        dma((2, NZ)),
        dma((2,)),
        dma((2,)),
    ]
    anywhere = pl.BlockSpec(memory_space=pl.ANY)
    in_vmem = pl.BlockSpec(memory_space=pltpu.VMEM)
    shapes = (queries.shape, keys.shape, values.shape)
    grads = pl.pallas_call(
        functools.partial(kernel, tps, heads),
        out_shape=tuple(pltpu.VMEM(shape, BF16) for shape in shapes),
        in_specs=[pl.BlockSpec(memory_space=pltpu.SMEM)] + [anywhere] * 4,
        out_specs=(in_vmem,) * 3,
        scratch_shapes=scratch,
        compiler_params=pltpu.CompilerParams(
            collective_id=0, has_side_effects=True, vmem_limit_bytes=56 * 1024 * 1024
        ),
    )(span_order, queries, keys, values, output_gradient)
    return tuple(
        pl.pallas_call(
            put_out,
            out_shape=tuple(jax.ShapeDtypeStruct(shape, BF16) for shape in shapes),
            in_specs=[in_vmem] * 3,
            out_specs=(anywhere,) * 3,
            scratch_shapes=[dma((3,))],
            compiler_params=pltpu.CompilerParams(vmem_limit_bytes=2 * 1024 * 1024),
        )(*grads)
    )


def put_out(a, b, c, x, y, z, sems):
    copies = [
        pltpu.make_async_copy(src, dst, sems.at[i])
        for i, (src, dst) in enumerate(((a, x), (b, y), (c, z)))
    ]
    for copy in copies:
        copy.start()
    for copy in copies:
        copy.wait()


def solution(mesh):
    return jax.shard_map(
        body,
        mesh=mesh,
        in_specs=(
            P("ctx", "tp"),
            P(("ctx", "tp"), None),
            P(("ctx", "tp"), None),
            P("ctx", "tp"),
            P(),
        ),
        out_specs=(P("ctx", "tp"), P(("ctx", "tp"), None), P(("ctx", "tp"), None)),
        check_vma=False,
    )
```

```python
import functools
import math

import jax
import jax.numpy as jnp
from jax import lax
from jax.experimental import pallas as pl
from jax.experimental.pallas import tpu as pltpu
from jax.sharding import PartitionSpec as P

HEAD = 128
SPAN = 64
KV_HEADS = 8
NY = 4
NZ = 4
SCALE = HEAD**-0.5
EXPO = SCALE * math.log2(math.e)
NEG = -1e30
ZT_FIRST = ((0, 0), (0, 1), (0, 2), (0, 3))
AG_RELAY = ()
INNER_AHEAD = 1
QUERY_CUT = 2
Z_FIRST = ()
RS_RELAY = ()
POINTS = {'early': (('zt', 1, 0), ('zt', 1, 1, 0), ('zt', 1, 2, 0), ('zt', 1, 3, 0)), 'first': (('pair', 0, 0), ('send', 1, 0, 0)), 'second': (('pair', 1, 0),), 'third': (('zt', 1, 1, 1), ('zt', 1, 2, 1), ('zt', 1, 3, 1)), 'score': {0: (('send', 1, 1, 0), ('send', 1, 0, 1)), 1: (('send', 1, 2, 0),), 2: (('send', 1, 3, 0), ('send', 1, 1, 1)), 3: (('send', 1, 2, 1), ('send', 1, 3, 1))}, 'stats': (('inner', 1, 0),), 'value': {}, 'delta': (), 'key': {0: (('total', 1, 3),), 1: (('total', 1, 2),), 2: (('total', 1, 1),), 3: (('total', 1, 0),)}, 'keys': (), 'last': (('total', 0, 2),), 'end': (('total', 0, 1), ('total', 0, 0)), 'middle': (('total', 0, 3),)}
MESH = pl.DeviceIdType.MESH
F32 = jnp.float32
BF16 = jnp.bfloat16


def dot(a, b):
    return jnp.dot(a, b, preferred_element_type=F32)


def kernel(
    tps,
    heads,
    span_hbm,
    q_hbm,
    k_hbm,
    v_hbm,
    g_hbm,
    dq_out,
    k_out,
    v_out,
    span,
    kvst,
    kv,
    qs,
    gs,
    qn,
    gn,
    qt,
    gt,
    klo_s,
    kc_s,
    vlo_s,
    vc_s,
    s_s,
    d_s,
    ds_s,
    s3_s,
    d3_s,
    st,
    st_in,
    cs,
    dl,
    dl_in,
    dqt,
    dk3,
    dqsend,
    dqrecv,
    out,
    ro,
    ry,
    zs,
    kvr,
    rzv,
    loc,
    zt_s,
    zt_r,
    ysem_s,
    ysem_r,
    pair_s,
    pair_r,
    yo_s,
    yo_r,
    yf_s,
    yf_r,
    zr_s,
    zr_r,
    zv_s,
    zv_r,
):
    rows = heads * SPAN
    toks = 2 * SPAN
    tt = toks // tps
    c = lax.axis_index("ctx")
    t = lax.axis_index("tp")
    core = lax.rem(c, 2)
    y = lax.rem(c // 2, NY)
    z = c // (2 * NY)

    def ctx_of(zz, yy, cc):
        return (zz * NY + yy) * 2 + cc

    y_up, y_dn, y_op = lax.rem(y + 1, NY), lax.rem(y + 3, NY), lax.rem(y + 2, NY)
    dev_yu, dev_yd = (ctx_of(z, y_up, core), t), (ctx_of(z, y_dn, core), t)
    dev_yo = (ctx_of(z, y_op, core), t)
    dev_pair = (ctx_of(z, y, 1 - core), t)

    def remote(src, dst, send, recv, device):
        return pltpu.make_async_remote_copy(
            src_ref=src,
            dst_ref=dst,
            send_sem=send,
            recv_sem=recv,
            device_id=device,
            device_id_type=MESH,
        )

    def landed(ref, sem):
        pltpu.make_async_copy(ref, ref, sem).wait()

    own_rows = pl.ds(pl.multiple_of(t * tt, tt), tt)
    own_cols = pl.ds(pl.multiple_of(t * HEAD, HEAD), HEAD)

    def fetch(w, hbm):
        for g in range(tps):
            pltpu.make_async_copy(
                hbm.at[:, pl.ds(g * HEAD, HEAD)], kvst.at[w, g], loc.at[w]
            ).start()
        pltpu.make_async_copy(
            hbm.at[:, own_cols], kv.at[z, y, w, own_rows], zt_r.at[w, z]
        ).start()

    fetch(0, k_hbm)
    span_copy = pltpu.make_async_copy(span_hbm, span, loc.at[4])
    span_copy.start()

    def z_of(gi):
        return lax.rem(z + gi + (gi // 2) * (1 - 2 * (gi % 2)), NZ)

    def greet(device):
        pl.semaphore_signal(barrier, inc=1, device_id=device, device_id_type=MESH)

    barrier = pltpu.get_barrier_semaphore()
    for gi in range(NZ):
        for o in range(1 if gi == 0 else 0, tps):
            greet((ctx_of(z_of(gi), y, core), lax.rem(t + o, tps)))
    for device in (dev_yu, dev_yd, dev_yo, dev_pair):
        greet(device)
    fetch(1, v_hbm)
    landed(kvst.at[0], loc.at[0])
    pl.semaphore_wait(barrier, NZ * tps - 1 + 4)

    def zt_send(w, gi):
        if (w, gi) == (1, 0):
            landed(kvst.at[1], loc.at[1])
        for o in range(1 if gi == 0 else 0, tps):
            to = lax.rem(t + o, tps)
            device = (ctx_of(z_of(gi), y, core), to)
            remote(
                kvst.at[w, to], kv.at[z, y, w, own_rows], zt_s.at[w, gi], zt_r.at[w, z], device
            ).start()

    for w, gi in ZT_FIRST:
        zt_send(w, gi)
    for h in range(heads):
        cols = pl.ds(h * HEAD, HEAD)
        pltpu.make_async_copy(q_hbm.at[:, cols], qs.at[0, h], loc.at[2]).start()
        pltpu.make_async_copy(g_hbm.at[:, cols], gs.at[0, h], loc.at[3]).start()
    pairs = [(qs, remote(qs.at[0], qs.at[1], pair_s.at[0], pair_r.at[0], dev_pair))]
    pairs.append((gs, remote(gs.at[0], gs.at[1], pair_s.at[1], pair_r.at[1], dev_pair)))
    q_copy, g_copy = pairs[0][1], pairs[1][1]

    def pair_send(w, gi):
        landed(pairs[w][0].at[0], loc.at[2 + w])
        pairs[w][1].start()

    span_copy.wait()

    def spans(cc):
        s0, s1 = span[2 * cc], span[2 * cc + 1]
        return s0 > s1, jnp.minimum(s0, s1)

    devs = (c, ctx_of(z, y, 1 - core))
    flips, lows = zip(*[spans(d) for d in devs])

    def prepare(a, src, normal, turned):
        first = src[a, :, 0:SPAN, :].reshape(rows, HEAD)
        second = src[a, :, SPAN : 2 * SPAN, :].reshape(rows, HEAD)
        lo = jnp.where(flips[a], second, first)
        hi = jnp.where(flips[a], first, second)
        normal[a, :, 0:HEAD] = lo
        normal[a, :, HEAD : 2 * HEAD] = hi
        turned[a, 0:HEAD, :] = lo.T
        turned[a, HEAD : 2 * HEAD, :] = hi.T

    low, high = pl.ds(0, SPAN), pl.ds(SPAN, SPAN)

    def y_send(w, gi):
        zg = z_of(gi)
        b = kv.at[zg, y, w]
        landed(b, zt_r.at[w, zg])
        remote(b, b, ysem_s.at[w, gi, 0], ysem_r.at[w, gi, 0], dev_yu).start()
        remote(b, b, ysem_s.at[w, gi, 1], ysem_r.at[w, gi, 1], dev_yd).start()
        if (w, gi) not in AG_RELAY:
            remote(b, b, ysem_s.at[w, gi, 2], ysem_r.at[w, gi, 2], dev_yo).start()

    def y_relay(w, gi):
        zg = z_of(gi)
        landed(kv.at[zg, y_dn, w], ysem_r.at[w, gi, 0])
        b = kv.at[zg, y_dn, w, low]
        remote(b, b, ysem_s.at[w, gi, 2], ysem_r.at[w, gi, 2], dev_yu).start()
        landed(kv.at[zg, y_up, w], ysem_r.at[w, gi, 1])
        b = kv.at[zg, y_up, w, high]
        remote(b, b, ysem_s.at[w, gi, 3], ysem_r.at[w, gi, 3], dev_yd).start()

    def y_done(w, gi):
        zg = z_of(gi)
        if (w, gi) in AG_RELAY:
            landed(kv.at[zg, y_op, w, low], ysem_r.at[w, gi, 2])
            landed(kv.at[zg, y_op, w, high], ysem_r.at[w, gi, 3])
        else:
            landed(kv.at[zg, y_dn, w], ysem_r.at[w, gi, 0])
            landed(kv.at[zg, y_up, w], ysem_r.at[w, gi, 1])
            landed(kv.at[zg, y_op, w], ysem_r.at[w, gi, 2])

    steps = {}

    def act(name, g=None):
        for step, w, gi, *only in POINTS[name] if g is None else POINTS[name].get(g, ()):
            todo = functools.partial(steps[step], w, gi)
            if only:
                pl.when(core == only[0])(todo)
            else:
                todo()

    def point(name, i):
        for g in POINTS[name]:
            pl.when(i == g)(functools.partial(act, name, g))

    def at(gi, todo):
        for g in range(NZ):
            pl.when(gi == g)(functools.partial(todo, g))

    steps["relay"], steps["send"] = y_relay, y_send
    steps["zt"], steps["pair"] = zt_send, pair_send
    act("early")
    y_send(0, 0)
    act("first")
    prepare(0, qs, qn, qt)
    y_send(0, 1)
    y_send(0, 2)
    act("second")

    def lohi(zg, yy, w):
        first, second = kv[zg, yy, w, 0:SPAN, :], kv[zg, yy, w, SPAN : 2 * SPAN, :]
        flip, _ = spans(ctx_of(zg, yy, core))
        return jnp.where(flip, second, first), jnp.where(flip, first, second)

    key_i = lax.broadcasted_iota(jnp.int32, (SPAN, rows), 0)
    tok_i = lax.rem(lax.broadcasted_iota(jnp.int32, (SPAN, rows), 1), SPAN)
    hidden = key_i > tok_i

    s3 = jnp.where(hidden, NEG, dot(lohi(z, y, 0)[0], qt[0, 0:HEAD, :]))
    s3_s[...] = s3
    m3 = jnp.max(s3, axis=0, keepdims=True)
    e3 = jnp.exp2((s3 - m3) * EXPO)
    none = jnp.full((1, rows), NEG, F32)
    zero = jnp.zeros((1, rows), F32)
    for a in range(2):
        st[a, 0:1, :] = none if a else m3
        st[a, 1:2, :] = zero if a else jnp.sum(e3, axis=0, keepdims=True)
        st[a, 2:3, :] = none
        st[a, 3:8, :] = jnp.zeros((5, rows), F32)
    y_send(0, 3)
    act("third")
    prepare(0, gs, gn, gt)
    q_copy.wait_recv()
    prepare(1, qs, qn, qt)
    def picks(zg, a):
        return [spans(ctx_of(zg, yy, core))[1] < lows[a] for yy in range(NY)]

    def block(yy):
        return slice(yy * SPAN, (yy + 1) * SPAN)

    def split(zg, w, lo_s, cat_s, gi):
        pairs = [lohi(zg, yy, w) for yy in range(NY)]
        for yy in range(NY):
            lo_s[gi, block(yy), :] = pairs[yy][0]
        for a in range(2):
            pick = picks(zg, a)
            for yy in range(NY):
                lo, hi = pairs[yy]
                none_ = jnp.zeros_like(lo)
                cat_s[gi, a, block(yy), 0:HEAD] = jnp.where(pick[yy], lo, none_)
                cat_s[gi, a, block(yy), HEAD : 2 * HEAD] = jnp.where(pick[yy], none_, hi)

    def column_sum(x):
        return jnp.sum(x, axis=0, keepdims=True)

    def scores(gi):
        zg = z_of(gi)
        split(zg, 0, klo_s, kc_s, gi)
        for a in range(2):
            pick = picks(zg, a)
            s1 = dot(klo_s[gi], qt[a, HEAD : 2 * HEAD, :])
            s2 = dot(kc_s[gi, a], qt[a])
            s_s[gi, a, 0] = s1
            parts = []
            for yy in range(NY):
                part = s2[block(yy), :]
                if a == 0:
                    here = jnp.logical_and(zg == z, yy == y)
                    part = jnp.where(jnp.logical_and(hidden, here), NEG, part)
                s_s[gi, a, 1, block(yy), :] = part
                parts.append(part)
            m_lo, l_lo, m_hi, l_hi = (st[a, i : i + 1, :] for i in range(4))
            n_lo, n_hi = m_lo, jnp.maximum(m_hi, jnp.max(s1, axis=0, keepdims=True))
            for yy in range(NY):
                top = jnp.max(parts[yy], axis=0, keepdims=True)
                n_lo = jnp.maximum(n_lo, jnp.where(pick[yy], top, none))
                n_hi = jnp.maximum(n_hi, jnp.where(pick[yy], none, top))
            l_lo = l_lo * jnp.exp2((m_lo - n_lo) * EXPO)
            l_hi = l_hi * jnp.exp2((m_hi - n_hi) * EXPO)
            l_hi = l_hi + column_sum(jnp.exp2((s1 - n_hi) * EXPO))
            for yy in range(NY):
                e2 = jnp.exp2((parts[yy] - jnp.where(pick[yy], n_lo, n_hi)) * EXPO)
                total = column_sum(e2)
                l_lo = l_lo + jnp.where(pick[yy], total, zero)
                l_hi = l_hi + jnp.where(pick[yy], zero, total)
            for i, x in enumerate((n_lo, l_lo, n_hi, l_hi)):
                st[a, i : i + 1, :] = x

    def inner(gi):
        split(z_of(gi), 1, vlo_s, vc_s, gi)
        for a in range(2):
            d_s[gi, a, 0] = dot(vlo_s[gi], gt[a, HEAD : 2 * HEAD, :])
            d_s[gi, a, 1] = dot(vc_s[gi, a], gt[a])

    def inner_now(w, gi):
        y_done(w, gi)
        inner(gi)

    steps["inner"] = inner_now

    def score_step(gi, carry):
        at(gi, functools.partial(y_done, 0))
        scores(gi)
        point("score", gi)
        return carry

    lax.fori_loop(0, NZ, score_step, 0)

    st_copy = remote(st, st_in, pair_s.at[2], pair_r.at[2], dev_pair)
    st_copy.start()
    dqt[...] = jnp.zeros_like(dqt)
    g_copy.wait_recv()
    prepare(1, gs, gn, gt)
    act("stats")
    st_copy.wait_recv()
    for a in range(2):
        for at_ in (0, 2):
            m0, l0 = (st[a, at_ + i : at_ + i + 1, :] for i in range(2))
            m1, l1 = (st_in[1 - a, at_ + i : at_ + i + 1, :] for i in range(2))
            m = jnp.maximum(m0, m1)
            total = l0 * jnp.exp2((m0 - m) * EXPO) + l1 * jnp.exp2((m1 - m) * EXPO)
            cs[a, at_ : at_ + 1, :] = m
            cs[a, at_ + 1 : at_ + 2, :] = 1.0 / total

    def prob_of(s, m, inv):
        return jnp.exp2((s - m) * EXPO) * inv

    d3_s[...] = dot(lohi(z, y, 1)[0], gt[0, 0:HEAD, :])
    p3 = prob_of(s3_s[...], cs[0, 0:1, :], cs[0, 1:2, :])
    s3_s[...] = p3
    dk3[1] = dot(p3.astype(BF16), gn[0, :, 0:HEAD])
    for a in range(2):
        dl[a, 0:1, :] = zero if a else column_sum(p3 * d3_s[...])
        dl[a, 1:8, :] = jnp.zeros((7, rows), F32)

    def collect(gi, w, tiles, wide):
        zg = z_of(gi)
        dlo, dhi = [None] * NY, [None] * NY
        for a in range(2):
            x1, x2 = tiles(a)
            pick = picks(zg, a)
            one = dot(x1, wide[a, :, HEAD : 2 * HEAD])
            two = dot(x2, wide[a])
            for yy in range(NY):
                left, right = two[block(yy), 0:HEAD], two[block(yy), HEAD : 2 * HEAD]
                none_ = jnp.zeros_like(left)
                new_lo = one[block(yy), :] + jnp.where(pick[yy], left, none_)
                new_hi = jnp.where(pick[yy], none_, right)
                if a == 0:
                    here = jnp.logical_and(zg == z, yy == y)
                    dlo[yy], dhi[yy] = new_lo + jnp.where(here, dk3[w], none_), new_hi
                else:
                    dlo[yy], dhi[yy] = dlo[yy] + new_lo, dhi[yy] + new_hi
        for yy in range(NY):
            flip, _ = spans(ctx_of(zg, yy, core))
            out[zg, yy, w, 0:SPAN, :] = jnp.where(flip, dhi[yy], dlo[yy]).astype(BF16)
            out[zg, yy, w, SPAN : 2 * SPAN, :] = jnp.where(flip, dlo[yy], dhi[yy]).astype(BF16)

    def value_grads(gi):
        zg = z_of(gi)

        def tiles(a):
            pick = picks(zg, a)
            m_lo, i_lo, m_hi, i_hi = (cs[a, i : i + 1, :] for i in range(4))
            p1 = prob_of(s_s[gi, a, 0], m_hi, i_hi)
            s_s[gi, a, 0] = p1
            w2 = []
            for yy in range(NY):
                p2 = prob_of(
                    s_s[gi, a, 1, block(yy), :],
                    jnp.where(pick[yy], m_lo, m_hi),
                    jnp.where(pick[yy], i_lo, i_hi),
                )
                s_s[gi, a, 1, block(yy), :] = p2
                w2.append(p2.astype(BF16))
            return p1.astype(BF16), jnp.concatenate(w2, axis=0)

        collect(gi, 1, tiles, gn)

    def deltas(gi):
        zg = z_of(gi)
        for a in range(2):
            pick = picks(zg, a)
            e_lo = dl[a, 0:1, :]
            e_hi = dl[a, 1:2, :] + column_sum(s_s[gi, a, 0] * d_s[gi, a, 0])
            for yy in range(NY):
                part = column_sum(s_s[gi, a, 1, block(yy), :] * d_s[gi, a, 1, block(yy), :])
                e_lo = e_lo + jnp.where(pick[yy], part, zero)
                e_hi = e_hi + jnp.where(pick[yy], zero, part)
            dl[a, 0:1, :] = e_lo
            dl[a, 1:2, :] = e_hi

    def score_grad(p, d, delta):
        return (p * (d - delta) * SCALE).astype(BF16)

    def key_grads(gi):
        zg = z_of(gi)

        def tiles(a):
            pick = picks(zg, a)
            e_lo, e_hi = (dl[a, i : i + 1, :] + dl_in[1 - a, i : i + 1, :] for i in range(2))
            ds_s[gi, a, 0] = score_grad(s_s[gi, a, 0], d_s[gi, a, 0], e_hi)
            for yy in range(NY):
                ds_s[gi, a, 1, block(yy), :] = score_grad(
                    s_s[gi, a, 1, block(yy), :],
                    d_s[gi, a, 1, block(yy), :],
                    jnp.where(pick[yy], e_lo, e_hi),
                )
            return ds_s[gi, a, 0], ds_s[gi, a, 1]

        collect(gi, 0, tiles, qn)

    def query_step(gi, carry):
        for a in range(2):
            dqt[a] += dot(kc_s[gi, a].T, ds_s[gi, a, 1])
            dqt[a, HEAD : 2 * HEAD, :] += dot(klo_s[gi].T, ds_s[gi, a, 0])
        return carry

    def plus(a, b):
        return (a.astype(F32) + b.astype(F32)).astype(BF16)

    def ry_first(w, gi):
        zg = z_of(gi)
        if (w, gi) in RS_RELAY:
            remote(
                out.at[zg, y_op, w, low], ro.at[gi, w, low], yo_s.at[w, gi, 0], yo_r.at[w, gi, 0], dev_yu
            ).start()
            remote(
                out.at[zg, y_op, w, high], ro.at[gi, w, high], yo_s.at[w, gi, 1], yo_r.at[w, gi, 1], dev_yd
            ).start()
        else:
            ry_near(w, gi, 0)
            ry_near(w, gi, 1)
            remote(
                out.at[zg, y_op, w], ro.at[gi, w], yo_s.at[w, gi, 0], yo_r.at[w, gi, 0], dev_yo
            ).start()

    def ry_near(w, gi, i):
        b = out.at[z_of(gi), (y_up, y_dn)[i], w]
        remote(
            b, ry.at[gi, i, w], yf_s.at[w, gi, i], yf_r.at[w, gi, i], (dev_yu, dev_yd)[i]
        ).start()

    def ry_forward(w, gi):
        zg = z_of(gi)
        landed(ro.at[gi, w, low], yo_r.at[w, gi, 0])
        out[zg, y_up, w, low] = plus(out[zg, y_up, w, low], ro[gi, w, low])
        ry_near(w, gi, 0)
        landed(ro.at[gi, w, high], yo_r.at[w, gi, 1])
        out[zg, y_dn, w, high] = plus(out[zg, y_dn, w, high], ro[gi, w, high])
        ry_near(w, gi, 1)

    def ry_total(w, gi):
        zg = z_of(gi)
        landed(ry.at[gi, 0, w], yf_r.at[w, gi, 0])
        landed(ry.at[gi, 1, w], yf_r.at[w, gi, 1])
        total = out[zg, y, w].astype(F32) + ry[gi, 0, w].astype(F32) + ry[gi, 1, w].astype(F32)
        if (w, gi) not in RS_RELAY:
            landed(ro.at[gi, w], yo_r.at[w, gi, 0])
            total = total + ro[gi, w].astype(F32)
        zs[gi, w] = total.astype(BF16)
        for o in range(1 if gi == 0 else 0, tps):
            to = lax.rem(t + o, tps)
            to_rows = pl.ds(pl.multiple_of(to * tt, tt), tt)
            device = (ctx_of(zg, y, core), to)
            remote(
                zs.at[gi, w, to_rows], kvr.at[z, w, t], zr_s.at[w, gi], zr_r.at[w, z], device
            ).start()

    steps["forward"], steps["total"] = ry_forward, ry_total

    def z_first(gi):
        zg = z_of(gi)
        remote(
            out.at[zg, :, 1], rzv.at[gi - 1], zv_s.at[gi - 1], zv_r.at[gi - 1], (ctx_of(zg, y, core), t)
        ).start()

    def z_merge(w, gi):
        for i in range(2):
            landed(rzv.at[i], zv_r.at[i])
        for yy in range(NY):
            total = out[z, yy, w].astype(F32) + rzv[0, yy].astype(F32) + rzv[1, yy].astype(F32)
            out[z, yy, w] = total.astype(BF16)
        ry_first(w, gi)

    steps["merge"], steps["open"] = z_merge, ry_first

    def value_step(i, carry):
        gi = NZ - 1 - i
        value_grads(gi)
        for g in range(1 if Z_FIRST else 0, NZ):
            pl.when(gi == g)(
                functools.partial(z_first, g) if g in Z_FIRST else functools.partial(ry_first, 1, g)
            )
        return carry

    lax.fori_loop(0, NZ, value_step, 0)

    def delta_step(gi, carry):
        for g in range(INNER_AHEAD, NZ):
            pl.when(gi == g)(functools.partial(y_done, 1, g))

        @pl.when(gi >= INNER_AHEAD)
        def _():
            inner(gi)

        deltas(gi)
        return carry

    lax.fori_loop(0, NZ, delta_step, 0)

    dl_copy = remote(dl, dl_in, pair_s.at[4], pair_r.at[4], dev_pair)
    dl_copy.start()
    act("delta")
    dl_copy.wait_recv()
    ds3 = score_grad(s3_s[...], d3_s[...], dl[0, 0:1, :] + dl_in[1, 0:1, :])
    dk3[0] = dot(ds3, qn[0, :, 0:HEAD])
    dqt[0, 0:HEAD, :] = dot(lohi(z, y, 0)[0].T, ds3)

    def key_step(i, carry):
        gi = NZ - 1 - i
        key_grads(gi)
        at(gi, functools.partial(ry_first, 0))
        point("key", i)
        return carry

    lax.fori_loop(0, NZ, key_step, 0)

    act("keys")
    lax.fori_loop(0, QUERY_CUT, query_step, 0)
    act("middle")
    lax.fori_loop(QUERY_CUT, NZ, query_step, 0)
    dqsend[...] = dqt[1].astype(BF16)
    dq_copy = remote(dqsend, dqrecv, pair_s.at[3], pair_r.at[3], dev_pair)
    dq_copy.start()
    act("last")
    act("end")
    dq_copy.wait_recv()
    total_q = dqt[0] + dqrecv[...].astype(F32)
    lo, hi = total_q[0:HEAD, :].T.astype(BF16), total_q[HEAD : 2 * HEAD, :].T.astype(BF16)
    first, second = jnp.where(flips[0], hi, lo), jnp.where(flips[0], lo, hi)
    for h in range(heads):
        dq_out[0:SPAN, h * HEAD : (h + 1) * HEAD] = first[h * SPAN : (h + 1) * SPAN, :]
        dq_out[SPAN : 2 * SPAN, h * HEAD : (h + 1) * HEAD] = second[h * SPAN : (h + 1) * SPAN, :]
    for w in range(2):
        kvr[z, w, t] = zs[0, w, own_rows]

    for copy in (q_copy, g_copy, st_copy, dl_copy, dq_copy):
        copy.wait_send()
    whole = kv.at[0, 0, 0]
    half = kv.at[0, 0, 0, low]
    pieces = [kvst.at[0, pl.ds(0, tps - 1)]] + [kvst.at[0]] * (NZ - 1)
    for w in range(2):
        for gi in range(NZ):
            landed(pieces[gi], zt_s.at[w, gi])
            straight = w == 0 or gi not in Z_FIRST
            if straight:
                landed(pieces[gi], zr_s.at[w, gi])
            relay = (w, gi) in AG_RELAY
            for i in range(4 if relay else 3):
                landed(half if relay and i >= 2 else whole, ysem_s.at[w, gi, i])
            relay = (w, gi) in RS_RELAY
            for i in range(2 if relay else 1):
                if straight:
                    landed(half if relay else whole, yo_s.at[w, gi, i])
            for i in range(2):
                if straight:
                    landed(whole, yf_s.at[w, gi, i])
    for i in range(len(Z_FIRST)):
        landed(rzv.at[i], zv_s.at[i])
    for w, result in ((1, v_out), (0, k_out)):
        parts = [gi for gi in (3, 2, 1, 0) if w == 0 or gi not in Z_FIRST]
        for gi in parts:
            landed(pieces[gi], zr_r.at[w, z_of(gi)])
        for g in range(tps):
            total = sum(kvr[z_of(gi), w, g].astype(F32) for gi in parts)
            result[:, g * HEAD : (g + 1) * HEAD] = total.astype(BF16)


def body(queries, keys, values, output_gradient, span_order):
    tps = lax.axis_size("tp")
    toks, width = queries.shape
    heads = width // HEAD
    rows = heads * SPAN
    tt = keys.shape[0]
    vmem = pltpu.VMEM
    half = (toks, HEAD)
    block = (2, *half)
    group = NY * SPAN
    dma = pltpu.SemaphoreType.DMA
    scratch = [
        pltpu.SMEM(span_order.shape, jnp.int32),
        vmem((2, tps, tt, HEAD), BF16),
        vmem((NZ, NY, *block), BF16),
        vmem((2, heads, *half), BF16),
        vmem((2, heads, *half), BF16),
        vmem((2, rows, 2 * HEAD), BF16),
        vmem((2, rows, 2 * HEAD), BF16),
        vmem((2, 2 * HEAD, rows), BF16),
        vmem((2, 2 * HEAD, rows), BF16),
        vmem((NZ, group, HEAD), BF16),
        vmem((NZ, 2, group, 2 * HEAD), BF16),
        vmem((NZ, group, HEAD), BF16),
        vmem((NZ, 2, group, 2 * HEAD), BF16),
        vmem((NZ, 2, 2, group, rows), F32),
        vmem((NZ, 2, 2, group, rows), F32),
        vmem((NZ, 2, 2, group, rows), BF16),
        vmem((SPAN, rows), F32),
        vmem((SPAN, rows), F32),
        vmem((2, 8, rows), F32),
        vmem((2, 8, rows), F32),
        vmem((2, 8, rows), F32),
        vmem((2, 8, rows), F32),
        vmem((2, 8, rows), F32),
        vmem((2, 2 * HEAD, rows), F32),
        vmem((2, SPAN, HEAD), F32),
        vmem((2 * HEAD, rows), BF16),
        vmem((2 * HEAD, rows), BF16),
        vmem((NZ, NY, *block), BF16),
        vmem((NZ, *block), BF16),
        vmem((NZ, 2, *block), BF16),
        vmem((NZ, *block), BF16),
        vmem((NZ, 2, tps, tt, HEAD), BF16),
        vmem((2, NY, *half), BF16),
        dma((5,)),
        dma((2, NZ)),
        dma((2, NZ)),
        dma((2, NZ, 4)),
        dma((2, NZ, 4)),
        dma((5,)),
        dma((5,)),
        dma((2, NZ, 2)),
        dma((2, NZ, 2)),
        dma((2, NZ, 2)),
        dma((2, NZ, 2)),
        dma((2, NZ)),
        dma((2, NZ)),
        dma((2,)),
        dma((2,)),
    ]
    anywhere = pl.BlockSpec(memory_space=pl.ANY)
    in_vmem = pl.BlockSpec(memory_space=pltpu.VMEM)
    shapes = (queries.shape, keys.shape, values.shape)
    grads = pl.pallas_call(
        functools.partial(kernel, tps, heads),
        out_shape=tuple(pltpu.VMEM(shape, BF16) for shape in shapes),
        in_specs=[anywhere] * 5,
        out_specs=(in_vmem,) * 3,
        scratch_shapes=scratch,
        compiler_params=pltpu.CompilerParams(
            collective_id=0, has_side_effects=True, vmem_limit_bytes=56 * 1024 * 1024
        ),
    )(span_order, queries, keys, values, output_gradient)
    return tuple(
        pl.pallas_call(
            put_out,
            out_shape=tuple(jax.ShapeDtypeStruct(shape, BF16) for shape in shapes),
            in_specs=[in_vmem] * 3,
            out_specs=(anywhere,) * 3,
            scratch_shapes=[dma((3,))],
            compiler_params=pltpu.CompilerParams(vmem_limit_bytes=2 * 1024 * 1024),
        )(*grads)
    )


def put_out(a, b, c, x, y, z, sems):
    copies = [
        pltpu.make_async_copy(src, dst, sems.at[i])
        for i, (src, dst) in enumerate(((a, x), (b, y), (c, z)))
    ]
    for copy in copies:
        copy.start()
    for copy in copies:
        copy.wait()


def solution(mesh):
    return jax.shard_map(
        body,
        mesh=mesh,
        in_specs=(
            P("ctx", "tp"),
            P(("ctx", "tp"), None),
            P(("ctx", "tp"), None),
            P("ctx", "tp"),
            P(),
        ),
        out_specs=(P("ctx", "tp"), P(("ctx", "tp"), None), P(("ctx", "tp"), None)),
        check_vma=False,
    )
```

```python
import functools
import math

import jax
import jax.numpy as jnp
from jax import lax
from jax.experimental import pallas as pl
from jax.experimental.pallas import tpu as pltpu
from jax.sharding import PartitionSpec as P

HEAD = 128
SPAN = 64
KV_HEADS = 8
NY = 4
NZ = 4
SCALE = HEAD**-0.5
EXPO = SCALE * math.log2(math.e)
NEG = -1e30
ZT_FIRST = ((0, 0), (0, 1), (0, 2), (0, 3))
AG_RELAY = ()
INNER_AHEAD = 1
QUERY_CUT = 2
Z_FIRST = ()
RS_RELAY = ()
POINTS = {'early': (('zt', 1, 0), ('zt', 1, 1, 0), ('zt', 1, 2, 0), ('zt', 1, 3, 0)), 'first': (('pair', 0, 0), ('send', 1, 0, 0)), 'second': (('pair', 1, 0),), 'third': (('zt', 1, 1, 1), ('zt', 1, 2, 1), ('zt', 1, 3, 1)), 'score': {0: (('send', 1, 1, 0), ('send', 1, 0, 1)), 1: (('send', 1, 2, 0),), 2: (('send', 1, 3, 0), ('send', 1, 1, 1)), 3: (('send', 1, 2, 1), ('send', 1, 3, 1))}, 'stats': (('inner', 1, 0),), 'value': {}, 'delta': (), 'key': {0: (('total', 1, 3),), 1: (('total', 1, 2),), 2: (('total', 1, 1),), 3: (('total', 1, 0),)}, 'keys': (), 'last': (('total', 0, 2),), 'end': (('total', 0, 1), ('total', 0, 0)), 'middle': (('total', 0, 3),)}
MESH = pl.DeviceIdType.MESH
F32 = jnp.float32
BF16 = jnp.bfloat16


def dot(a, b):
    return jnp.dot(a, b, preferred_element_type=F32)


def kernel(
    tps,
    heads,
    span_hbm,
    q_hbm,
    k_hbm,
    v_hbm,
    g_hbm,
    dq_out,
    k_out,
    v_out,
    span,
    kvst,
    kv,
    qs,
    gs,
    qn,
    gn,
    qt,
    gt,
    klo_s,
    kc_s,
    vlo_s,
    vc_s,
    s_s,
    d_s,
    ds_s,
    s3_s,
    d3_s,
    st,
    st_in,
    cs,
    dl,
    dl_in,
    dqt,
    dk3,
    dqsend,
    dqrecv,
    out,
    ro,
    ry,
    zs,
    kvr,
    rzv,
    loc,
    zt_s,
    zt_r,
    ysem_s,
    ysem_r,
    pair_s,
    pair_r,
    yo_s,
    yo_r,
    yf_s,
    yf_r,
    zr_s,
    zr_r,
    zv_s,
    zv_r,
):
    rows = heads * SPAN
    toks = 2 * SPAN
    tt = toks // tps
    c = lax.axis_index("ctx")
    t = lax.axis_index("tp")
    core = lax.rem(c, 2)
    y = lax.rem(c // 2, NY)
    z = c // (2 * NY)

    def ctx_of(zz, yy, cc):
        return (zz * NY + yy) * 2 + cc

    y_up, y_dn, y_op = lax.rem(y + 1, NY), lax.rem(y + 3, NY), lax.rem(y + 2, NY)
    dev_yu, dev_yd = (ctx_of(z, y_up, core), t), (ctx_of(z, y_dn, core), t)
    dev_yo = (ctx_of(z, y_op, core), t)
    dev_pair = (ctx_of(z, y, 1 - core), t)

    def remote(src, dst, send, recv, device):
        return pltpu.make_async_remote_copy(
            src_ref=src,
            dst_ref=dst,
            send_sem=send,
            recv_sem=recv,
            device_id=device,
            device_id_type=MESH,
        )

    def landed(ref, sem):
        pltpu.make_async_copy(ref, ref, sem).wait()

    own_rows = pl.ds(pl.multiple_of(t * tt, tt), tt)
    own_cols = pl.ds(pl.multiple_of(t * HEAD, HEAD), HEAD)

    def fetch(w, hbm):
        for g in range(tps):
            pltpu.make_async_copy(
                hbm.at[:, pl.ds(g * HEAD, HEAD)], kvst.at[w, g], loc.at[w]
            ).start()
        pltpu.make_async_copy(
            hbm.at[:, own_cols], kv.at[z, y, w, own_rows], zt_r.at[w, z]
        ).start()

    fetch(0, k_hbm)
    span_copy = pltpu.make_async_copy(span_hbm, span, loc.at[4])
    span_copy.start()

    def z_of(gi):
        return lax.rem(z + gi + (gi // 2) * (1 - 2 * (gi % 2)), NZ)

    def greet(device):
        pl.semaphore_signal(barrier, inc=1, device_id=device, device_id_type=MESH)

    barrier = pltpu.get_barrier_semaphore()
    for gi in range(NZ):
        for o in range(1 if gi == 0 else 0, tps):
            greet((ctx_of(z_of(gi), y, core), lax.rem(t + o, tps)))
    for device in (dev_yu, dev_yd, dev_yo, dev_pair):
        greet(device)
    landed(kvst.at[0], loc.at[0])
    pl.semaphore_wait(barrier, NZ * tps - 1 + 4)

    def zt_send(w, gi):
        if (w, gi) == (1, 0):
            landed(kvst.at[1], loc.at[1])
        for o in range(1 if gi == 0 else 0, tps):
            to = lax.rem(t + o, tps)
            device = (ctx_of(z_of(gi), y, core), to)
            remote(
                kvst.at[w, to], kv.at[z, y, w, own_rows], zt_s.at[w, gi], zt_r.at[w, z], device
            ).start()

    for w, gi in ZT_FIRST:
        zt_send(w, gi)
    fetch(1, v_hbm)
    for h in range(heads):
        cols = pl.ds(h * HEAD, HEAD)
        pltpu.make_async_copy(q_hbm.at[:, cols], qs.at[0, h], loc.at[2]).start()
        pltpu.make_async_copy(g_hbm.at[:, cols], gs.at[0, h], loc.at[3]).start()
    pairs = [(qs, remote(qs.at[0], qs.at[1], pair_s.at[0], pair_r.at[0], dev_pair))]
    pairs.append((gs, remote(gs.at[0], gs.at[1], pair_s.at[1], pair_r.at[1], dev_pair)))
    q_copy, g_copy = pairs[0][1], pairs[1][1]

    def pair_send(w, gi):
        landed(pairs[w][0].at[0], loc.at[2 + w])
        pairs[w][1].start()

    span_copy.wait()

    def spans(cc):
        s0, s1 = span[2 * cc], span[2 * cc + 1]
        return s0 > s1, jnp.minimum(s0, s1)

    devs = (c, ctx_of(z, y, 1 - core))
    flips, lows = zip(*[spans(d) for d in devs])

    def prepare(a, src, normal, turned):
        first = src[a, :, 0:SPAN, :].reshape(rows, HEAD)
        second = src[a, :, SPAN : 2 * SPAN, :].reshape(rows, HEAD)
        lo = jnp.where(flips[a], second, first)
        hi = jnp.where(flips[a], first, second)
        normal[a, :, 0:HEAD] = lo
        normal[a, :, HEAD : 2 * HEAD] = hi
        turned[a, 0:HEAD, :] = lo.T
        turned[a, HEAD : 2 * HEAD, :] = hi.T

    low, high = pl.ds(0, SPAN), pl.ds(SPAN, SPAN)

    def y_send(w, gi):
        zg = z_of(gi)
        b = kv.at[zg, y, w]
        landed(b, zt_r.at[w, zg])
        remote(b, b, ysem_s.at[w, gi, 0], ysem_r.at[w, gi, 0], dev_yu).start()
        remote(b, b, ysem_s.at[w, gi, 1], ysem_r.at[w, gi, 1], dev_yd).start()
        if (w, gi) not in AG_RELAY:
            remote(b, b, ysem_s.at[w, gi, 2], ysem_r.at[w, gi, 2], dev_yo).start()

    def y_relay(w, gi):
        zg = z_of(gi)
        landed(kv.at[zg, y_dn, w], ysem_r.at[w, gi, 0])
        b = kv.at[zg, y_dn, w, low]
        remote(b, b, ysem_s.at[w, gi, 2], ysem_r.at[w, gi, 2], dev_yu).start()
        landed(kv.at[zg, y_up, w], ysem_r.at[w, gi, 1])
        b = kv.at[zg, y_up, w, high]
        remote(b, b, ysem_s.at[w, gi, 3], ysem_r.at[w, gi, 3], dev_yd).start()

    def y_done(w, gi):
        zg = z_of(gi)
        if (w, gi) in AG_RELAY:
            landed(kv.at[zg, y_op, w, low], ysem_r.at[w, gi, 2])
            landed(kv.at[zg, y_op, w, high], ysem_r.at[w, gi, 3])
        else:
            landed(kv.at[zg, y_dn, w], ysem_r.at[w, gi, 0])
            landed(kv.at[zg, y_up, w], ysem_r.at[w, gi, 1])
            landed(kv.at[zg, y_op, w], ysem_r.at[w, gi, 2])

    steps = {}

    def act(name, g=None):
        for step, w, gi, *only in POINTS[name] if g is None else POINTS[name].get(g, ()):
            todo = functools.partial(steps[step], w, gi)
            if only:
                pl.when(core == only[0])(todo)
            else:
                todo()

    def point(name, i):
        for g in POINTS[name]:
            pl.when(i == g)(functools.partial(act, name, g))

    def at(gi, todo):
        for g in range(NZ):
            pl.when(gi == g)(functools.partial(todo, g))

    steps["relay"], steps["send"] = y_relay, y_send
    steps["zt"], steps["pair"] = zt_send, pair_send
    act("early")
    y_send(0, 0)
    act("first")
    prepare(0, qs, qn, qt)
    y_send(0, 1)
    y_send(0, 2)
    act("second")

    def lohi(zg, yy, w):
        first, second = kv[zg, yy, w, 0:SPAN, :], kv[zg, yy, w, SPAN : 2 * SPAN, :]
        flip, _ = spans(ctx_of(zg, yy, core))
        return jnp.where(flip, second, first), jnp.where(flip, first, second)

    key_i = lax.broadcasted_iota(jnp.int32, (SPAN, rows), 0)
    tok_i = lax.rem(lax.broadcasted_iota(jnp.int32, (SPAN, rows), 1), SPAN)
    hidden = key_i > tok_i

    s3 = jnp.where(hidden, NEG, dot(lohi(z, y, 0)[0], qt[0, 0:HEAD, :]))
    s3_s[...] = s3
    m3 = jnp.max(s3, axis=0, keepdims=True)
    e3 = jnp.exp2((s3 - m3) * EXPO)
    none = jnp.full((1, rows), NEG, F32)
    zero = jnp.zeros((1, rows), F32)
    for a in range(2):
        st[a, 0:1, :] = none if a else m3
        st[a, 1:2, :] = zero if a else jnp.sum(e3, axis=0, keepdims=True)
        st[a, 2:3, :] = none
        st[a, 3:8, :] = jnp.zeros((5, rows), F32)
    y_send(0, 3)
    act("third")
    prepare(0, gs, gn, gt)
    q_copy.wait_recv()
    prepare(1, qs, qn, qt)
    def picks(zg, a):
        return [spans(ctx_of(zg, yy, core))[1] < lows[a] for yy in range(NY)]

    def block(yy):
        return slice(yy * SPAN, (yy + 1) * SPAN)

    def split(zg, w, lo_s, cat_s, gi):
        pairs = [lohi(zg, yy, w) for yy in range(NY)]
        for yy in range(NY):
            lo_s[gi, block(yy), :] = pairs[yy][0]
        for a in range(2):
            pick = picks(zg, a)
            for yy in range(NY):
                lo, hi = pairs[yy]
                none_ = jnp.zeros_like(lo)
                cat_s[gi, a, block(yy), 0:HEAD] = jnp.where(pick[yy], lo, none_)
                cat_s[gi, a, block(yy), HEAD : 2 * HEAD] = jnp.where(pick[yy], none_, hi)

    def column_sum(x):
        return jnp.sum(x, axis=0, keepdims=True)

    def scores(gi):
        zg = z_of(gi)
        split(zg, 0, klo_s, kc_s, gi)
        for a in range(2):
            pick = picks(zg, a)
            s1 = dot(klo_s[gi], qt[a, HEAD : 2 * HEAD, :])
            s2 = dot(kc_s[gi, a], qt[a])
            s_s[gi, a, 0] = s1
            parts = []
            for yy in range(NY):
                part = s2[block(yy), :]
                if a == 0:
                    here = jnp.logical_and(zg == z, yy == y)
                    part = jnp.where(jnp.logical_and(hidden, here), NEG, part)
                s_s[gi, a, 1, block(yy), :] = part
                parts.append(part)
            m_lo, l_lo, m_hi, l_hi = (st[a, i : i + 1, :] for i in range(4))
            n_lo, n_hi = m_lo, jnp.maximum(m_hi, jnp.max(s1, axis=0, keepdims=True))
            for yy in range(NY):
                top = jnp.max(parts[yy], axis=0, keepdims=True)
                n_lo = jnp.maximum(n_lo, jnp.where(pick[yy], top, none))
                n_hi = jnp.maximum(n_hi, jnp.where(pick[yy], none, top))
            l_lo = l_lo * jnp.exp2((m_lo - n_lo) * EXPO)
            l_hi = l_hi * jnp.exp2((m_hi - n_hi) * EXPO)
            l_hi = l_hi + column_sum(jnp.exp2((s1 - n_hi) * EXPO))
            for yy in range(NY):
                e2 = jnp.exp2((parts[yy] - jnp.where(pick[yy], n_lo, n_hi)) * EXPO)
                total = column_sum(e2)
                l_lo = l_lo + jnp.where(pick[yy], total, zero)
                l_hi = l_hi + jnp.where(pick[yy], zero, total)
            for i, x in enumerate((n_lo, l_lo, n_hi, l_hi)):
                st[a, i : i + 1, :] = x

    def inner(gi):
        split(z_of(gi), 1, vlo_s, vc_s, gi)
        for a in range(2):
            d_s[gi, a, 0] = dot(vlo_s[gi], gt[a, HEAD : 2 * HEAD, :])
            d_s[gi, a, 1] = dot(vc_s[gi, a], gt[a])

    def inner_now(w, gi):
        y_done(w, gi)
        inner(gi)

    steps["inner"] = inner_now

    def score_step(gi, carry):
        at(gi, functools.partial(y_done, 0))
        scores(gi)
        point("score", gi)
        return carry

    lax.fori_loop(0, NZ, score_step, 0)

    st_copy = remote(st, st_in, pair_s.at[2], pair_r.at[2], dev_pair)
    st_copy.start()
    dqt[...] = jnp.zeros_like(dqt)
    g_copy.wait_recv()
    prepare(1, gs, gn, gt)
    act("stats")
    st_copy.wait_recv()
    for a in range(2):
        for at_ in (0, 2):
            m0, l0 = (st[a, at_ + i : at_ + i + 1, :] for i in range(2))
            m1, l1 = (st_in[1 - a, at_ + i : at_ + i + 1, :] for i in range(2))
            m = jnp.maximum(m0, m1)
            total = l0 * jnp.exp2((m0 - m) * EXPO) + l1 * jnp.exp2((m1 - m) * EXPO)
            cs[a, at_ : at_ + 1, :] = m
            cs[a, at_ + 1 : at_ + 2, :] = 1.0 / total

    def prob_of(s, m, inv):
        return jnp.exp2((s - m) * EXPO) * inv

    d3_s[...] = dot(lohi(z, y, 1)[0], gt[0, 0:HEAD, :])
    p3 = prob_of(s3_s[...], cs[0, 0:1, :], cs[0, 1:2, :])
    s3_s[...] = p3
    dk3[1] = dot(p3.astype(BF16), gn[0, :, 0:HEAD])
    for a in range(2):
        dl[a, 0:1, :] = zero if a else column_sum(p3 * d3_s[...])
        dl[a, 1:8, :] = jnp.zeros((7, rows), F32)

    def collect(gi, w, tiles, wide):
        zg = z_of(gi)
        dlo, dhi = [None] * NY, [None] * NY
        for a in range(2):
            x1, x2 = tiles(a)
            pick = picks(zg, a)
            one = dot(x1, wide[a, :, HEAD : 2 * HEAD])
            two = dot(x2, wide[a])
            for yy in range(NY):
                left, right = two[block(yy), 0:HEAD], two[block(yy), HEAD : 2 * HEAD]
                none_ = jnp.zeros_like(left)
                new_lo = one[block(yy), :] + jnp.where(pick[yy], left, none_)
                new_hi = jnp.where(pick[yy], none_, right)
                if a == 0:
                    here = jnp.logical_and(zg == z, yy == y)
                    dlo[yy], dhi[yy] = new_lo + jnp.where(here, dk3[w], none_), new_hi
                else:
                    dlo[yy], dhi[yy] = dlo[yy] + new_lo, dhi[yy] + new_hi
        for yy in range(NY):
            flip, _ = spans(ctx_of(zg, yy, core))
            out[zg, yy, w, 0:SPAN, :] = jnp.where(flip, dhi[yy], dlo[yy]).astype(BF16)
            out[zg, yy, w, SPAN : 2 * SPAN, :] = jnp.where(flip, dlo[yy], dhi[yy]).astype(BF16)

    def value_grads(gi):
        zg = z_of(gi)

        def tiles(a):
            pick = picks(zg, a)
            m_lo, i_lo, m_hi, i_hi = (cs[a, i : i + 1, :] for i in range(4))
            p1 = prob_of(s_s[gi, a, 0], m_hi, i_hi)
            s_s[gi, a, 0] = p1
            w2 = []
            for yy in range(NY):
                p2 = prob_of(
                    s_s[gi, a, 1, block(yy), :],
                    jnp.where(pick[yy], m_lo, m_hi),
                    jnp.where(pick[yy], i_lo, i_hi),
                )
                s_s[gi, a, 1, block(yy), :] = p2
                w2.append(p2.astype(BF16))
            return p1.astype(BF16), jnp.concatenate(w2, axis=0)

        collect(gi, 1, tiles, gn)

    def deltas(gi):
        zg = z_of(gi)
        for a in range(2):
            pick = picks(zg, a)
            e_lo = dl[a, 0:1, :]
            e_hi = dl[a, 1:2, :] + column_sum(s_s[gi, a, 0] * d_s[gi, a, 0])
            for yy in range(NY):
                part = column_sum(s_s[gi, a, 1, block(yy), :] * d_s[gi, a, 1, block(yy), :])
                e_lo = e_lo + jnp.where(pick[yy], part, zero)
                e_hi = e_hi + jnp.where(pick[yy], zero, part)
            dl[a, 0:1, :] = e_lo
            dl[a, 1:2, :] = e_hi

    def score_grad(p, d, delta):
        return (p * (d - delta) * SCALE).astype(BF16)

    def key_grads(gi):
        zg = z_of(gi)

        def tiles(a):
            pick = picks(zg, a)
            e_lo, e_hi = (dl[a, i : i + 1, :] + dl_in[1 - a, i : i + 1, :] for i in range(2))
            ds_s[gi, a, 0] = score_grad(s_s[gi, a, 0], d_s[gi, a, 0], e_hi)
            for yy in range(NY):
                ds_s[gi, a, 1, block(yy), :] = score_grad(
                    s_s[gi, a, 1, block(yy), :],
                    d_s[gi, a, 1, block(yy), :],
                    jnp.where(pick[yy], e_lo, e_hi),
                )
            return ds_s[gi, a, 0], ds_s[gi, a, 1]

        collect(gi, 0, tiles, qn)

    def query_step(gi, carry):
        for a in range(2):
            dqt[a] += dot(kc_s[gi, a].T, ds_s[gi, a, 1])
            dqt[a, HEAD : 2 * HEAD, :] += dot(klo_s[gi].T, ds_s[gi, a, 0])
        return carry

    def plus(a, b):
        return (a.astype(F32) + b.astype(F32)).astype(BF16)

    def ry_first(w, gi):
        zg = z_of(gi)
        if (w, gi) in RS_RELAY:
            remote(
                out.at[zg, y_op, w, low], ro.at[gi, w, low], yo_s.at[w, gi, 0], yo_r.at[w, gi, 0], dev_yu
            ).start()
            remote(
                out.at[zg, y_op, w, high], ro.at[gi, w, high], yo_s.at[w, gi, 1], yo_r.at[w, gi, 1], dev_yd
            ).start()
        else:
            ry_near(w, gi, 0)
            ry_near(w, gi, 1)
            remote(
                out.at[zg, y_op, w], ro.at[gi, w], yo_s.at[w, gi, 0], yo_r.at[w, gi, 0], dev_yo
            ).start()

    def ry_near(w, gi, i):
        b = out.at[z_of(gi), (y_up, y_dn)[i], w]
        remote(
            b, ry.at[gi, i, w], yf_s.at[w, gi, i], yf_r.at[w, gi, i], (dev_yu, dev_yd)[i]
        ).start()

    def ry_forward(w, gi):
        zg = z_of(gi)
        landed(ro.at[gi, w, low], yo_r.at[w, gi, 0])
        out[zg, y_up, w, low] = plus(out[zg, y_up, w, low], ro[gi, w, low])
        ry_near(w, gi, 0)
        landed(ro.at[gi, w, high], yo_r.at[w, gi, 1])
        out[zg, y_dn, w, high] = plus(out[zg, y_dn, w, high], ro[gi, w, high])
        ry_near(w, gi, 1)

    def ry_total(w, gi):
        zg = z_of(gi)
        landed(ry.at[gi, 0, w], yf_r.at[w, gi, 0])
        landed(ry.at[gi, 1, w], yf_r.at[w, gi, 1])
        total = out[zg, y, w].astype(F32) + ry[gi, 0, w].astype(F32) + ry[gi, 1, w].astype(F32)
        if (w, gi) not in RS_RELAY:
            landed(ro.at[gi, w], yo_r.at[w, gi, 0])
            total = total + ro[gi, w].astype(F32)
        zs[gi, w] = total.astype(BF16)
        for o in range(1 if gi == 0 else 0, tps):
            to = lax.rem(t + o, tps)
            to_rows = pl.ds(pl.multiple_of(to * tt, tt), tt)
            device = (ctx_of(zg, y, core), to)
            remote(
                zs.at[gi, w, to_rows], kvr.at[z, w, t], zr_s.at[w, gi], zr_r.at[w, z], device
            ).start()

    steps["forward"], steps["total"] = ry_forward, ry_total

    def z_first(gi):
        zg = z_of(gi)
        remote(
            out.at[zg, :, 1], rzv.at[gi - 1], zv_s.at[gi - 1], zv_r.at[gi - 1], (ctx_of(zg, y, core), t)
        ).start()

    def z_merge(w, gi):
        for i in range(2):
            landed(rzv.at[i], zv_r.at[i])
        for yy in range(NY):
            total = out[z, yy, w].astype(F32) + rzv[0, yy].astype(F32) + rzv[1, yy].astype(F32)
            out[z, yy, w] = total.astype(BF16)
        ry_first(w, gi)

    steps["merge"], steps["open"] = z_merge, ry_first

    def value_step(i, carry):
        gi = NZ - 1 - i
        value_grads(gi)
        for g in range(1 if Z_FIRST else 0, NZ):
            pl.when(gi == g)(
                functools.partial(z_first, g) if g in Z_FIRST else functools.partial(ry_first, 1, g)
            )
        return carry

    lax.fori_loop(0, NZ, value_step, 0)

    def delta_step(gi, carry):
        for g in range(INNER_AHEAD, NZ):
            pl.when(gi == g)(functools.partial(y_done, 1, g))

        @pl.when(gi >= INNER_AHEAD)
        def _():
            inner(gi)

        deltas(gi)
        return carry

    lax.fori_loop(0, NZ, delta_step, 0)

    dl_copy = remote(dl, dl_in, pair_s.at[4], pair_r.at[4], dev_pair)
    dl_copy.start()
    act("delta")
    dl_copy.wait_recv()
    ds3 = score_grad(s3_s[...], d3_s[...], dl[0, 0:1, :] + dl_in[1, 0:1, :])
    dk3[0] = dot(ds3, qn[0, :, 0:HEAD])
    dqt[0, 0:HEAD, :] = dot(lohi(z, y, 0)[0].T, ds3)

    def key_step(i, carry):
        gi = NZ - 1 - i
        key_grads(gi)
        at(gi, functools.partial(ry_first, 0))
        point("key", i)
        return carry

    lax.fori_loop(0, NZ, key_step, 0)

    act("keys")
    lax.fori_loop(0, QUERY_CUT, query_step, 0)
    act("middle")
    lax.fori_loop(QUERY_CUT, NZ, query_step, 0)
    dqsend[...] = dqt[1].astype(BF16)
    dq_copy = remote(dqsend, dqrecv, pair_s.at[3], pair_r.at[3], dev_pair)
    dq_copy.start()
    act("last")
    act("end")
    dq_copy.wait_recv()
    total_q = dqt[0] + dqrecv[...].astype(F32)
    lo, hi = total_q[0:HEAD, :].T.astype(BF16), total_q[HEAD : 2 * HEAD, :].T.astype(BF16)
    first, second = jnp.where(flips[0], hi, lo), jnp.where(flips[0], lo, hi)
    for h in range(heads):
        dq_out[0:SPAN, h * HEAD : (h + 1) * HEAD] = first[h * SPAN : (h + 1) * SPAN, :]
        dq_out[SPAN : 2 * SPAN, h * HEAD : (h + 1) * HEAD] = second[h * SPAN : (h + 1) * SPAN, :]
    for w in range(2):
        kvr[z, w, t] = zs[0, w, own_rows]

    for copy in (q_copy, g_copy, st_copy, dl_copy, dq_copy):
        copy.wait_send()
    whole = kv.at[0, 0, 0]
    half = kv.at[0, 0, 0, low]
    pieces = [kvst.at[0, pl.ds(0, tps - 1)]] + [kvst.at[0]] * (NZ - 1)
    for w in range(2):
        for gi in range(NZ):
            landed(pieces[gi], zt_s.at[w, gi])
            straight = w == 0 or gi not in Z_FIRST
            if straight:
                landed(pieces[gi], zr_s.at[w, gi])
            relay = (w, gi) in AG_RELAY
            for i in range(4 if relay else 3):
                landed(half if relay and i >= 2 else whole, ysem_s.at[w, gi, i])
            relay = (w, gi) in RS_RELAY
            for i in range(2 if relay else 1):
                if straight:
                    landed(half if relay else whole, yo_s.at[w, gi, i])
            for i in range(2):
                if straight:
                    landed(whole, yf_s.at[w, gi, i])
    for i in range(len(Z_FIRST)):
        landed(rzv.at[i], zv_s.at[i])
    for w, result in ((1, v_out), (0, k_out)):
        parts = [gi for gi in (3, 2, 1, 0) if w == 0 or gi not in Z_FIRST]
        for gi in parts:
            landed(pieces[gi], zr_r.at[w, z_of(gi)])
        for g in range(tps):
            total = sum(kvr[z_of(gi), w, g].astype(F32) for gi in parts)
            result[:, g * HEAD : (g + 1) * HEAD] = total.astype(BF16)


def body(queries, keys, values, output_gradient, span_order):
    tps = lax.axis_size("tp")
    toks, width = queries.shape
    heads = width // HEAD
    rows = heads * SPAN
    tt = keys.shape[0]
    vmem = pltpu.VMEM
    half = (toks, HEAD)
    block = (2, *half)
    group = NY * SPAN
    dma = pltpu.SemaphoreType.DMA
    scratch = [
        pltpu.SMEM(span_order.shape, jnp.int32),
        vmem((2, tps, tt, HEAD), BF16),
        vmem((NZ, NY, *block), BF16),
        vmem((2, heads, *half), BF16),
        vmem((2, heads, *half), BF16),
        vmem((2, rows, 2 * HEAD), BF16),
        vmem((2, rows, 2 * HEAD), BF16),
        vmem((2, 2 * HEAD, rows), BF16),
        vmem((2, 2 * HEAD, rows), BF16),
        vmem((NZ, group, HEAD), BF16),
        vmem((NZ, 2, group, 2 * HEAD), BF16),
        vmem((NZ, group, HEAD), BF16),
        vmem((NZ, 2, group, 2 * HEAD), BF16),
        vmem((NZ, 2, 2, group, rows), F32),
        vmem((NZ, 2, 2, group, rows), F32),
        vmem((NZ, 2, 2, group, rows), BF16),
        vmem((SPAN, rows), F32),
        vmem((SPAN, rows), F32),
        vmem((2, 8, rows), F32),
        vmem((2, 8, rows), F32),
        vmem((2, 8, rows), F32),
        vmem((2, 8, rows), F32),
        vmem((2, 8, rows), F32),
        vmem((2, 2 * HEAD, rows), F32),
        vmem((2, SPAN, HEAD), F32),
        vmem((2 * HEAD, rows), BF16),
        vmem((2 * HEAD, rows), BF16),
        vmem((NZ, NY, *block), BF16),
        vmem((NZ, *block), BF16),
        vmem((NZ, 2, *block), BF16),
        vmem((NZ, *block), BF16),
        vmem((NZ, 2, tps, tt, HEAD), BF16),
        vmem((2, NY, *half), BF16),
        dma((5,)),
        dma((2, NZ)),
        dma((2, NZ)),
        dma((2, NZ, 4)),
        dma((2, NZ, 4)),
        dma((5,)),
        dma((5,)),
        dma((2, NZ, 2)),
        dma((2, NZ, 2)),
        dma((2, NZ, 2)),
        dma((2, NZ, 2)),
        dma((2, NZ)),
        dma((2, NZ)),
        dma((2,)),
        dma((2,)),
    ]
    anywhere = pl.BlockSpec(memory_space=pl.ANY)
    in_vmem = pl.BlockSpec(memory_space=pltpu.VMEM)
    shapes = (queries.shape, keys.shape, values.shape)
    grads = pl.pallas_call(
        functools.partial(kernel, tps, heads),
        out_shape=tuple(pltpu.VMEM(shape, BF16) for shape in shapes),
        in_specs=[anywhere] * 5,
        out_specs=(in_vmem,) * 3,
        scratch_shapes=scratch,
        compiler_params=pltpu.CompilerParams(
            collective_id=0, has_side_effects=True, vmem_limit_bytes=56 * 1024 * 1024
        ),
    )(span_order, queries, keys, values, output_gradient)
    return tuple(
        pl.pallas_call(
            put_out,
            out_shape=tuple(jax.ShapeDtypeStruct(shape, BF16) for shape in shapes),
            in_specs=[in_vmem] * 3,
            out_specs=(anywhere,) * 3,
            scratch_shapes=[dma((3,))],
            compiler_params=pltpu.CompilerParams(vmem_limit_bytes=2 * 1024 * 1024),
        )(*grads)
    )


def put_out(a, b, c, x, y, z, sems):
    copies = [
        pltpu.make_async_copy(src, dst, sems.at[i])
        for i, (src, dst) in enumerate(((a, x), (b, y), (c, z)))
    ]
    for copy in copies:
        copy.start()
    for copy in copies:
        copy.wait()


def solution(mesh):
    return jax.shard_map(
        body,
        mesh=mesh,
        in_specs=(
            P("ctx", "tp"),
            P(("ctx", "tp"), None),
            P(("ctx", "tp"), None),
            P("ctx", "tp"),
            P(),
        ),
        out_specs=(P("ctx", "tp"), P(("ctx", "tp"), None), P(("ctx", "tp"), None)),
        check_vma=False,
    )
```
